256 devices in a mesh: grp: 32 (over z, y), rep: 8 (over x, core).
Axes of the slice: x: 4, y: 4, z: 8, core: 2. Of those that a mesh axis runs over, the one named last changes fastest.
Arguments:
- queries: bfloat16 [64, 8, 32, 128], P('grp', 'rep'), may hold values from -3.2 to 3.2
- passages: bfloat16 [2048, 8, 180, 128], P('grp', 'rep'), may hold values from -1.796875 to 1.796875
- lengths: int32 [2048, 8], P('grp', 'rep'), may hold values from 16 to 180
- cand_ids: int32 [64, 8, 64], P('grp', 'rep'), may hold values from 0 to 2047, as said below
- owner_map: int32 [8, 2048], P('rep'), may hold values from 0 to 2047, as said below
- teacher: float32 [64, 8, 64], P('grp', 'rep'), may hold values from -12 to 312
- weights: float32 [64, 8], P('grp', 'rep'), may hold values from 0.5 to 18
Outputs:
- loss: float32 [], replicated
- query_grad: float32 [64, 8, 32, 128], P('grp', 'rep')
- passage_grad: bfloat16 [2048, 8, 180, 128], P('grp', 'rep')
The draws below stay inside these ranges and needn't reach their ends.
Inputs may be any that keep to these rules, and one draw needn't show every extreme that they name: `cand_ids`: within each replica, the 128 candidates of the queries of one grp index have storage rows of which at most 8 (counted with repeats) lie in any one aligned block of 64 rows; in every draw, in each replica, one block receives exactly 8 from every grp index. `owner_map`: each row is a permutation of 0 to 2047.
All inputs are finite; a program needn't handle non-finite values.
Results may differ from the reference program's by a relative error of at most 0.0055.
Values may be sent and summed in bfloat16 or wider, within the bound.
A program may use at most 128 MiB of HBM per device.

```python
import math
import jax
import jax.numpy as jnp
from jax import lax

DIM = 128
QL = 32
PL = 180
NWAY = 64
Q_DEV = 2
P_DEV = 64
GROUPS = 32
REPS = 8
QUERIES = 64
PASSAGES = 2048


def routing(key):
    ref_count = Q_DEV * NWAY
    capacity = 2 * ref_count // GROUPS
    pool_size = GROUPS * capacity
    keys = jax.random.split(jax.random.fold_in(key, 7), 5)
    hot_owner = jax.random.randint(keys[0], (REPS,), 0, GROUPS)
    pool_owner = jnp.arange(pool_size, dtype=jnp.int32) // capacity
    priority = jax.random.randint(keys[1], (GROUPS, REPS, pool_size), 0, 1 << 20) * pool_size + jnp.arange(pool_size, dtype=jnp.int32)
    is_hot = pool_owner[None, None, :] == hot_owner[None, :, None]
    priority = jnp.where(is_hot, jnp.arange(pool_size, dtype=jnp.int32) - pool_size, priority)
    order = jnp.argsort(priority, axis=-1)[..., :ref_count]
    owners = pool_owner[order]
    shuffle_key = jax.random.randint(keys[2], (GROUPS, REPS, ref_count), 0, 1 << 20) * ref_count + jnp.arange(ref_count, dtype=jnp.int32)
    shuffle = jnp.argsort(shuffle_key, axis=-1)
    owners = jnp.take_along_axis(owners, shuffle, axis=-1)
    slot_rows = jax.random.randint(keys[3], (GROUPS, REPS, ref_count), 0, P_DEV)
    storage = owners * P_DEV + slot_rows
    perm_keys = jax.random.split(keys[4], REPS)
    owner_table = jax.vmap(lambda one_key: jax.random.permutation(one_key, P_DEV * GROUPS))(perm_keys).astype(jnp.int32)
    inverse = jnp.argsort(owner_table, axis=-1).astype(jnp.int32)
    wide_inverse = jnp.broadcast_to(inverse[None], (GROUPS, REPS, P_DEV * GROUPS))
    identity = jnp.take_along_axis(wide_inverse, storage, axis=-1)
    candidate_ids = identity.reshape(GROUPS, REPS, Q_DEV, NWAY).transpose(0, 2, 1, 3).reshape(GROUPS * Q_DEV, REPS, NWAY)
    return (candidate_ids.astype(jnp.int32), owner_table)


def draw_cand_ids(key, part):
    return routing(key)[0]


def draw_owner_map(key, part):
    return routing(key)[1]


def draw_queries(key, part):
    keys = jax.random.split(jax.random.fold_in(key, 11), 2)
    shape = (QUERIES, REPS, QL, DIM)
    normal_part = jnp.clip(jax.random.normal(keys[0], shape, jnp.float32), -3.5, 3.5)
    row_scale = jnp.exp(jax.random.uniform(keys[1], (QUERIES, REPS, 1, 1), jnp.float32, math.log(0.03), math.log(3.0)))
    return (0.3 * normal_part * row_scale).astype(jnp.bfloat16)


def draw_teacher(key, part):
    keys = jax.random.split(jax.random.fold_in(key, 13), 1)
    normal_part = 2.0 * jnp.clip(jax.random.normal(keys[0], (QUERIES, REPS, NWAY), jnp.float32), -6.0, 6.0)
    return normal_part


def draw_weights(key, part):
    keys = jax.random.split(jax.random.fold_in(key, 17), 1)
    query_index = jnp.arange(QUERIES, dtype=jnp.int32)[:, None]
    replica_index = jnp.arange(REPS, dtype=jnp.int32)[None, :]
    device_index = query_index // Q_DEV * REPS + replica_index
    ramp = 1.0 + 2.0 * device_index.astype(jnp.float32) / (GROUPS * REPS - 1)
    return jnp.exp(jax.random.uniform(keys[0], (QUERIES, REPS), jnp.float32, math.log(0.5), math.log(2.0))) * ramp


def place_ends(values, stream_key, low, largest):
    longest = values.shape.index(max(values.shape))
    spots = []
    for shift in (0, 1):
        where = [jax.random.randint(jax.random.fold_in(stream_key, axis), (), 0, length) for axis, length in enumerate(values.shape)]
        where[longest] = (where[longest] + shift) % values.shape[longest]
        spots.append(tuple(where))
    return values.at[spots[0]].set(low).at[spots[1]].set(largest)


def block_levels(key, shape, pieces, low, top_value):
    loudness = 1.0
    for position, shards_of in pieces:
        heights = jax.random.uniform(jax.random.fold_in(jax.random.fold_in(key, 6), position), (shards_of,), jnp.float32, low / len(pieces), top_value / len(pieces))
        loudness = loudness * jnp.repeat(jnp.exp(heights), shape[position] // shards_of).reshape((-1,) + (1,) * (len(shape) - 1 - position))
    return loudness


def gaussian(rng, extent, width, bound, shards=(), held_as=jnp.bfloat16):
    entries = width * jax.random.normal(rng, extent, jnp.float32)
    if shards:
        entries = entries * block_levels(rng, extent, shards, -0.22, 0.18)
    return jnp.clip(entries, -bound, bound).astype(held_as)


def setup_inputs(seed: int = 0) -> dict:
    seeds = jax.random.split(jax.random.key(seed), 8)
    return {
        "queries": draw_queries(jax.random.fold_in(seeds[7], 71), 0),
        "passages": gaussian(seeds[1], (PASSAGES, REPS, PL, DIM), 0.3, 1.796875, ((0, 32), (1, 8))),
        "lengths": place_ends(jax.random.randint(seeds[2], (PASSAGES, REPS), 16, PL + 1), jax.random.fold_in(seeds[2], 1), 16, PL).astype(jnp.int32),
        "cand_ids": draw_cand_ids(jax.random.fold_in(seeds[7], 71), 0),
        "owner_map": draw_owner_map(jax.random.fold_in(seeds[7], 71), 0),
        "teacher": draw_teacher(jax.random.fold_in(seeds[7], 71), 0),
        "weights": draw_weights(jax.random.fold_in(seeds[7], 71), 0),
    }


temper = 0.05


def rounded(values):
    return lax.optimization_barrier(values.astype(jnp.bfloat16)).astype(jnp.float32)


def token_softmax(products, lengths_used):
    usable = lax.broadcasted_iota(jnp.int32, products.shape, products.ndim - 1) < lengths_used[..., None, None]
    scaled = jnp.where(usable, products / temper, -1e30)
    highest = jnp.max(scaled, axis=-1, keepdims=True)
    powers = jnp.where(usable, jnp.exp(scaled - highest), 0.0)
    summed = jnp.sum(powers, axis=-1, keepdims=True)
    matched = temper * (highest[..., 0] + jnp.log(summed[..., 0]))
    return matched, powers / summed


def pair_terms(query_tokens, passage_tokens, lengths_used):
    products = jnp.einsum("id,cjd->cij", query_tokens.astype(jnp.float32), passage_tokens.astype(jnp.float32))
    matched, attention = token_softmax(products, lengths_used)
    return jnp.sum(matched, axis=-1), attention


def reference(queries, passages, lengths, cand_ids, owner_map, teacher, weights):
    query_count = queries.shape[0]
    replicas = queries.shape[1]

    def fetch_blocks(query_row, replica):
        storage_rows = owner_map[replica][cand_ids[query_row, replica]]
        return storage_rows, passages[storage_rows, replica], lengths[storage_rows, replica]

    def score_one(flat_index):
        query_row = flat_index // replicas
        replica = flat_index % replicas
        storage_rows, blocks, lengths_used = fetch_blocks(query_row, replica)
        return pair_terms(queries[query_row, replica], blocks, lengths_used)[0]

    student = lax.map(score_one, jnp.arange(query_count * replicas, dtype=jnp.int32))
    student = student.reshape(query_count, replicas, -1)
    log_student = jax.nn.log_softmax(student, axis=-1)
    log_teacher = jax.nn.log_softmax(teacher, axis=-1)
    teacher_prob = jnp.exp(log_teacher)
    divergence = jnp.sum(teacher_prob * (log_teacher - log_student), axis=-1)
    weight_sum = jnp.sum(weights)
    loss_value = jnp.sum(weights * divergence) / weight_sum
    score_grad = (query_count * replicas) * weights[..., None] / weight_sum * (jnp.exp(log_student) - teacher_prob)
    query_parts = []
    passage_parts = []
    for replica in range(replicas):
        def backward(accum_grad, query_row):
            storage_rows, blocks, lengths_used = fetch_blocks(query_row, replica)
            query_tokens = queries[query_row, replica]
            unused, attention = pair_terms(query_tokens, blocks, lengths_used)
            scaled_grad = rounded(score_grad[query_row, replica][:, None, None] * attention)
            pair_query = rounded(jnp.einsum("cij,cjd->cid", scaled_grad, blocks.astype(jnp.float32)))
            query_part = jnp.sum(pair_query, axis=0)
            pair_passage = rounded(jnp.einsum("cij,id->cjd", scaled_grad, query_tokens.astype(jnp.float32)))
            accum_grad = accum_grad.at[storage_rows].add(pair_passage)
            return accum_grad, query_part

        initial = jnp.zeros((passages.shape[0],) + passages.shape[2:], jnp.float32)
        summed, replica_grads = lax.scan(backward, initial, jnp.arange(query_count, dtype=jnp.int32))
        query_parts.append(replica_grads)
        passage_parts.append(summed.astype(jnp.bfloat16))
    return loss_value, jnp.stack(query_parts, axis=1), jnp.stack(passage_parts, axis=1)
```

```python
import functools

import jax
import jax.numpy as jnp
from jax import lax
from jax.experimental import pallas as pl
from jax.experimental.pallas import tpu as pltpu
from jax.sharding import PartitionSpec as P

MESH = pl.DeviceIdType.MESH
F32 = jnp.float32
BF16 = jnp.bfloat16
I32 = jnp.int32

temper = 0.05
SCALE2 = 20.0 * 1.4426950408889634
LANES = 128
CAP = 8
WIDE = 4
UNROLL = 8


def iota(shape, axis):
    return lax.broadcasted_iota(I32, shape, axis)


def to_row(col):
    n = col.shape[0]
    eye = iota((n, n), 0) == iota((n, n), 1)
    return jnp.sum(jnp.where(eye, col, jnp.zeros_like(col)), axis=0, keepdims=True)


def to_col(row):
    n = row.shape[1]
    eye = iota((n, n), 0) == iota((n, n), 1)
    return jnp.sum(jnp.where(eye, row, jnp.zeros_like(row)), axis=1, keepdims=True)


def pick(mask, values):
    return jnp.sum(jnp.where(mask, values, jnp.zeros_like(values)), axis=1, keepdims=True)


def step_kernel(
    G,
    R,
    NCH,
    cand_ref,
    omap_ref,
    q_ref,
    p_hbm,
    len_ref,
    teach_ref,
    w_ref,
    loss_ref,
    qgrad_ref,
    pgrad_hbm,
    p_v,
    q_all,
    x_s,
    y_r,
    v_s,
    v_r,
    g_r,
    wr,
    lr,
    meta_v,
    meta_s,
    m_v,
    att,
    u_v,
    slotr,
    loccol,
    sgq,
    sgl,
    qg_s,
    qg_r,
    acc,
    p_sem,
    meta_sem,
    out_sem,
    y_send,
    y_recv,
    q_send,
    q_recv,
    v_send,
    v_recv,
    g_send,
    g_recv,
    o_send,
    o_recv,
    w_send,
    w_recv,
    l_send,
    l_recv,
):
    me = lax.axis_index("grp")
    rep = lax.axis_index("rep")
    stored, token_len, dim = p_v.shape
    query_len = q_ref.shape[1]
    nslot = G * CAP

    def remote(src, dst, ssem, rsem, g, r):
        return pltpu.make_async_remote_copy(
            src_ref=src,
            dst_ref=dst,
            send_sem=ssem,
            recv_sem=rsem,
            device_id=(g, r),
            device_id_type=MESH,
        )

    def peers(body):
        def one(t, carry):
            body(lax.rem(me + t, G))
            return carry

        lax.fori_loop(1, G, one, 0)

    def reps(body):
        for t in range(1, R):
            body(lax.rem(rep + t, R))

    barrier = pltpu.get_barrier_semaphore()

    def greet(g):
        pl.semaphore_signal(barrier, inc=1, device_id=(g, rep), device_id_type=MESH)

    def greet_rep(r):
        pl.semaphore_signal(barrier, inc=1, device_id=(me, r), device_id_type=MESH)

    peers(greet)
    reps(greet_rep)
    p_copy = pltpu.make_async_copy(p_hbm, p_v, p_sem)
    p_copy.start()

    omap = omap_ref[...]
    count = omap.shape[1]
    wanted = to_col(cand_ref[...])
    pos = pick(wanted == iota((LANES, count), 1), jnp.broadcast_to(omap, (LANES, count)))
    pos_row = to_row(pos)
    owner = pos_row >> 6
    row1 = (pos_row & 63) + 1
    weights = w_ref[...]
    lane = iota((1, LANES), 1)
    half = lane >> 6
    mine_w = pick((lane & 63) == 0, weights)
    x_s[:, 0, :] = jnp.where(owner == iota((G, LANES), 0), row1, 0).astype(F32)
    x_s[:, 1, :] = jnp.broadcast_to(mine_w, (G, LANES))
    q_all[pl.ds(2 * me, 2)] = q_ref[...]
    y_r[me] = x_s[me]

    pl.semaphore_wait(barrier, G - 1 + R - 1)

    def send_y(g):
        remote(x_s.at[g], y_r.at[me], y_send.at[g], y_recv.at[me], g, rep).start()

    def send_q(g):
        remote(
            q_ref, q_all.at[pl.ds(2 * me, 2)], q_send.at[g], q_recv.at[me], g, rep
        ).start()

    peers(send_y)
    peers(send_q)

    def wait_y(g):
        remote(x_s.at[g], y_r.at[g], y_send.at[g], y_recv.at[g], g, rep).wait_recv()

    def wait_q(g):
        remote(
            q_ref, q_all.at[pl.ds(2 * g, 2)], q_send.at[g], q_recv.at[g], g, rep
        ).wait_recv()

    peers(wait_y)

    group_w = jnp.sum(y_r[:, 1, :], axis=0, keepdims=True)
    wr[rep] = group_w

    def send_w(r):
        remote(wr.at[rep], wr.at[rep], w_send.at[r], w_recv.at[rep], me, r).start()

    reps(send_w)

    y = y_r[:, 0, :].astype(I32)
    have = y > 0
    lower = (iota((LANES, LANES), 0) < iota((LANES, LANES), 1)).astype(BF16)
    before = jnp.dot(have.astype(F32).astype(BF16), lower, preferred_element_type=F32).astype(I32)
    ylane = iota((G, LANES), 1)
    code = jnp.where(have, (y << 7) | ylane, 0)
    codes = [pick(have & (before == k), code) for k in range(CAP)]
    for k in range(CAP):
        rk = jnp.where(codes[k] > 0, codes[k] & 127, -1)
        slotr[k] = jnp.broadcast_to(rk, (G, LANES))
    ecode = jnp.concatenate(codes, axis=0)
    ew = ecode >> 7
    er = ecode & 127
    es = jnp.concatenate([iota((G, 1), 0)] * CAP, axis=0)
    ew_row = to_row(ew)
    used_row = ew_row > 0
    same = (ew == ew_row) & used_row
    rank = jnp.sum(
        jnp.where(same & (iota((nslot, nslot), 1) < iota((nslot, nslot), 0)), 1, 0),
        axis=1,
        keepdims=True,
    )
    rank_row = to_row(rank)
    starts = used_row & ((rank_row & (WIDE - 1)) == 0) & (ew_row < ew)
    base = jnp.sum(jnp.where(starts, 1, 0), axis=1, keepdims=True)
    loc = jnp.where(ew > 0, (base + (rank >> 2)) * WIDE + (rank & (WIDE - 1)), -1)
    loccol[...] = jnp.broadcast_to(loc, (nslot, LANES))
    packed = (ew << 12) | (es << 7) | er
    for b in range(WIDE):
        hit = loc == iota((nslot, LANES), 1) * WIDE + b
        meta_v[b : b + 1, :] = jnp.sum(jnp.where(hit, packed, 0), axis=0, keepdims=True)
    loc_row = to_row(loc)
    for h in range(nslot // LANES):
        meta_v[WIDE + h : WIDE + h + 1, :] = loc_row[:, h * LANES : (h + 1) * LANES]
    plane = iota((nslot, LANES), 1) + 1
    begin = (ew > 0) & ((rank & (WIDE - 1)) == 0)
    first = jnp.sum(jnp.where(begin & (ew < plane), 1, 0), axis=0, keepdims=True)
    held = jnp.sum(jnp.where(begin & (ew == plane), 1, 0), axis=0, keepdims=True)
    meta_v[6:7, :] = jnp.where(held > 0, first + 1, 0)
    meta_v[7:8, :] = jnp.zeros((1, LANES), I32)
    meta_copy = pltpu.make_async_copy(meta_v, meta_s, meta_sem)
    meta_copy.start()
    m_v[...] = jnp.zeros_like(m_v)
    meta_copy.wait()
    p_copy.wait()
    peers(wait_q)

    def query_of(b, ch):
        return q_all[(meta_s[b, ch] >> 6) & (2 * G - 1)]

    def passage_of(ch):
        return jnp.maximum((meta_s[0, ch] >> 12) - 1, 0)

    token = iota((token_len, LANES), 0)

    def forward(ch):
        pid = passage_of(ch)
        queries = jnp.concatenate([query_of(b, ch) for b in range(WIDE)], axis=0)
        x = lax.dot_general(
            p_v[pid], queries, (((1,), (1,)), ((), ())), preferred_element_type=F32
        )
        x = jnp.where(token < len_ref[0, pid], x, -1e30)
        highest = jnp.max(x, axis=0, keepdims=True)
        powers = jnp.exp2((x - highest) * SCALE2)
        summed = jnp.sum(powers, axis=0, keepdims=True)
        att[ch] = (powers * (1.0 / summed)).astype(BF16)
        return highest + temper * jnp.log(summed)

    def forward_group(g, carry):
        rows = [forward(g * UNROLL + u) for u in range(UNROLL)]
        m_v[pl.ds(pl.multiple_of(g * UNROLL, UNROLL), UNROLL), :] = jnp.concatenate(rows, axis=0)
        return carry

    lax.fori_loop(0, NCH // UNROLL, forward_group, 0)

    matched = m_v[...]
    block = iota((LANES, LANES), 1) >> 5
    loc_cols = loccol[...]
    scores = jnp.zeros((nslot, 1), F32)
    for b in range(WIDE):
        row = to_row(pick(block == b, matched))
        hit = loc_cols == iota((nslot, LANES), 1) * WIDE + b
        scores += pick(hit, jnp.broadcast_to(row, (nslot, LANES)))
    score_rows = jnp.zeros((G, LANES), F32)
    for k in range(CAP):
        score_rows += jnp.where(slotr[k] == ylane, scores[k * G : (k + 1) * G, :], 0.0)
    v_s[:, 0, :] = score_rows
    v_r[me] = v_s[me]

    def send_v(g):
        remote(v_s.at[g], v_r.at[me], v_send.at[g], v_recv.at[me], g, rep).start()

    peers(send_v)

    def lift(ch):
        u = lax.dot_general(
            att[ch], p_v[passage_of(ch)], (((0,), (0,)), ((), ())), preferred_element_type=F32
        )
        u_v[pl.ds(ch * WIDE, WIDE)] = u.astype(BF16).reshape(WIDE, query_len, dim)

    def lift_group(g, carry):
        for u in range(UNROLL):
            lift(g * UNROLL + u)
        return carry

    lax.fori_loop(0, NCH // UNROLL, lift_group, 0)

    def wait_v(g):
        remote(v_s.at[g], v_r.at[g], v_send.at[g], v_recv.at[g], g, rep).wait_recv()

    def wait_w(r):
        remote(wr.at[r], wr.at[r], w_send.at[r], w_recv.at[r], me, r).wait_recv()

    peers(wait_v)
    reps(wait_w)

    def log_softmax(values):
        top = [jnp.max(jnp.where(half == h, values, -3e38), axis=1, keepdims=True) for h in (0, 1)]
        shifted = values - jnp.where(half == 0, top[0], top[1])
        e = jnp.exp(shifted)
        total = [pick(half == h, e) for h in (0, 1)]
        return shifted - jnp.log(jnp.where(half == 0, total[0], total[1]))

    log_student = log_softmax(jnp.sum(v_r[...], axis=0))
    log_teacher = log_softmax(teach_ref[...])
    teacher_prob = jnp.exp(log_teacher)
    weight_sum = jnp.sum(wr[...], axis=0)
    scale_all = 2.0 * G * R
    score_grad = scale_all * weights / weight_sum * (jnp.exp(log_student) - teacher_prob)
    part = jnp.sum(
        weights * (teacher_prob * (log_teacher - log_student)), axis=1, keepdims=True
    )
    g_r[me] = jnp.concatenate([score_grad, jnp.broadcast_to(part, (1, LANES))], axis=0)

    def send_g(g):
        remote(g_r.at[me], g_r.at[me], g_send.at[g], g_recv.at[me], g, rep).start()

    def wait_g(g):
        remote(g_r.at[g], g_r.at[g], g_send.at[g], g_recv.at[g], g, rep).wait_recv()

    peers(send_g)
    peers(wait_g)

    lr[rep] = jnp.sum(g_r[:, 1, :], axis=0, keepdims=True)

    def send_l(r):
        remote(lr.at[rep], lr.at[rep], l_send.at[r], l_recv.at[rep], me, r).start()

    reps(send_l)

    grads = g_r[:, 0, :]
    by_slot = []
    for k in range(CAP):
        rk = slotr[k]
        col = pick(rk == ylane, grads)
        by_slot.append(col)
        sgq[:, k, :] = jnp.where(rk < 64, col, 0.0)
        sgq[:, CAP + k, :] = jnp.where(rk >= 64, col, 0.0)

    def query_sum(s):
        scales = sgq[s]
        one = jnp.zeros((query_len, dim), F32)
        two = jnp.zeros((query_len, dim), F32)
        for k in range(CAP):
            e = k * G + s
            at = jnp.maximum(meta_s[WIDE + e // LANES, lax.rem(e, LANES)], 0)
            u = u_v[at].astype(F32)
            one += scales[k : k + 1, :] * u
            two += scales[CAP + k : CAP + k + 1, :] * u
        return one.astype(BF16), two.astype(BF16)

    def send_qg(t, carry):
        s = lax.rem(me + t, G)
        one, two = query_sum(s)
        qg_s[s, 0] = one
        qg_s[s, 1] = two
        remote(qg_s.at[s], qg_r.at[me], o_send.at[s], o_recv.at[me], s, rep).start()
        return carry

    lax.fori_loop(1, G, send_qg, 0)
    one, two = query_sum(me)
    qg_r[me, 0] = one
    qg_r[me, 1] = two

    sg_row = to_row(jnp.concatenate(by_slot, axis=0))
    loc_rows = jnp.concatenate(
        [meta_v[WIDE + h : WIDE + h + 1, :] for h in range(nslot // LANES)], axis=1
    )
    for b in range(WIDE):
        hit = loc_rows == iota((LANES, nslot), 0) * WIDE + b
        col = pick(hit, jnp.broadcast_to(sg_row, (LANES, nslot)))
        sgl[:, b, :] = jnp.broadcast_to(col, (LANES, LANES))

    acc[...] = jnp.zeros_like(acc)

    def back(ch):
        scales = sgl[ch]
        scaled = jnp.concatenate(
            [
                (query_of(b, ch).astype(F32) * scales[b : b + 1, :]).astype(BF16)
                for b in range(WIDE)
            ],
            axis=0,
        )
        product = jnp.dot(att[ch], scaled, preferred_element_type=F32)
        follows = (meta_s[0, ch] >> 12) == (meta_s[0, ch + 1] >> 12)
        total = product + acc[...] * jnp.where(follows, 1.0, 0.0)
        acc[...] = total
        att[ch] = total.astype(BF16)

    def back_group(i, carry):
        g = NCH // UNROLL - 1 - i
        for u in range(UNROLL):
            back(g * UNROLL + UNROLL - 1 - u)
        return carry

    lax.fori_loop(0, NCH // UNROLL, back_group, 0)

    def place(p, carry):
        mark = meta_s[6, p]
        p_v[p] = att[jnp.maximum(mark - 1, 0)] * jnp.where(mark > 0, 1.0, 0.0).astype(BF16)
        return carry

    lax.fori_loop(0, stored, place, 0)
    out_copy = pltpu.make_async_copy(p_v, pgrad_hbm, out_sem)
    out_copy.start()

    def wait_l(r):
        remote(lr.at[r], lr.at[r], l_send.at[r], l_recv.at[r], me, r).wait_recv()

    reps(wait_l)
    loss_ref[...] = jnp.sum(lr[...], axis=0) / weight_sum

    def wait_o(g):
        remote(qg_s.at[g], qg_r.at[g], o_send.at[g], o_recv.at[g], g, rep).wait_recv()

    peers(wait_o)

    def add(o, carry):
        return carry + qg_r[o].astype(F32)

    qgrad_ref[...] = lax.fori_loop(0, G, add, jnp.zeros(qgrad_ref.shape, F32))

    def drain(g):
        remote(x_s.at[g], y_r.at[g], y_send.at[g], y_recv.at[g], g, rep).wait_send()
        remote(q_ref, q_all.at[pl.ds(2 * g, 2)], q_send.at[g], q_recv.at[g], g, rep).wait_send()
        remote(v_s.at[g], v_r.at[g], v_send.at[g], v_recv.at[g], g, rep).wait_send()
        remote(g_r.at[g], g_r.at[g], g_send.at[g], g_recv.at[g], g, rep).wait_send()
        remote(qg_s.at[g], qg_r.at[g], o_send.at[g], o_recv.at[g], g, rep).wait_send()

    def drain_rep(r):
        remote(wr.at[r], wr.at[r], w_send.at[r], w_recv.at[r], me, r).wait_send()
        remote(lr.at[r], lr.at[r], l_send.at[r], l_recv.at[r], me, r).wait_send()

    peers(drain)
    reps(drain_rep)
    out_copy.wait()


def on_device(G, R, queries, passages, lengths, cand_ids, owner_map, teacher, weights):
    query_local, _, query_len, dim = queries.shape
    stored, _, token_len, _ = passages.shape
    chunks = (G * CAP + (WIDE - 1) * stored) // WIDE
    NCH = -(-chunks // UNROLL) * UNROLL
    vmem = pl.BlockSpec(memory_space=pltpu.VMEM)
    smem = pl.BlockSpec(memory_space=pltpu.SMEM)
    hbm = pl.BlockSpec(memory_space=pl.ANY)
    dma = pltpu.SemaphoreType.DMA
    shape = jax.ShapeDtypeStruct
    loss, qgrad, pgrad = pl.pallas_call(
        functools.partial(step_kernel, G, R, NCH),
        out_shape=(
            shape((1, LANES), F32),
            shape((query_local, query_len, dim), F32),
            shape((stored, token_len, dim), BF16),
        ),
        in_specs=[vmem, vmem, vmem, hbm, smem, vmem, vmem],
        out_specs=(vmem, vmem, hbm),
        scratch_shapes=[
            pltpu.VMEM((stored, token_len, dim), BF16),
            pltpu.VMEM((query_local * G, query_len, dim), BF16),
            pltpu.VMEM((G, 2, LANES), F32),
            pltpu.VMEM((G, 2, LANES), F32),
            pltpu.VMEM((G, 1, LANES), F32),
            pltpu.VMEM((G, 1, LANES), F32),
            pltpu.VMEM((G, 2, LANES), F32),
            pltpu.VMEM((R, 1, LANES), F32),
            pltpu.VMEM((R, 1, LANES), F32),
            pltpu.VMEM((8, LANES), I32),
            pltpu.SMEM((8, LANES), I32),
            pltpu.VMEM((LANES, LANES), F32),
            pltpu.VMEM((NCH, token_len, LANES), BF16),
            pltpu.VMEM((NCH * WIDE, query_len, dim), BF16),
            pltpu.VMEM((CAP, G, LANES), I32),
            pltpu.VMEM((G * CAP, LANES), I32),
            pltpu.VMEM((G, 2 * CAP, LANES), F32),
            pltpu.VMEM((LANES, WIDE, LANES), F32),
            pltpu.VMEM((G, query_local, query_len, dim), BF16),
            pltpu.VMEM((G, query_local, query_len, dim), BF16),
            pltpu.VMEM((token_len, dim), F32),
            dma,
            dma,
            dma,
        ]
        + [dma((G,))] * 10
        + [dma((R,))] * 4,
        compiler_params=pltpu.CompilerParams(
            collective_id=0, has_side_effects=True, vmem_limit_bytes=56 * 1024 * 1024
        ),
    )(
        cand_ids.reshape(1, LANES),
        owner_map,
        queries.reshape(query_local, query_len, dim),
        passages.reshape(stored, token_len, dim),
        lengths.reshape(1, stored),
        teacher.reshape(1, LANES),
        jnp.repeat(weights.reshape(query_local), LANES // query_local).reshape(1, LANES),
    )
    return loss[0, 0], qgrad[:, None], pgrad[:, None]


def solution(mesh):
    G, R = mesh.shape["grp"], mesh.shape["rep"]
    in_specs = (
        P("grp", "rep", None, None),
        P("grp", "rep", None, None),
        P("grp", "rep"),
        P("grp", "rep", None),
        P("rep", None),
        P("grp", "rep", None),
        P("grp", "rep"),
    )
    out_specs = (P(), P("grp", "rep", None, None), P("grp", "rep", None, None))
    return jax.shard_map(
        functools.partial(on_device, G, R),
        mesh=mesh,
        in_specs=in_specs,
        out_specs=out_specs,
        check_vma=False,
    )
```

```python
import functools

import jax
import jax.numpy as jnp
from jax import lax
from jax.experimental import pallas as pl
from jax.experimental.pallas import tpu as pltpu
from jax.sharding import PartitionSpec as P

MESH = pl.DeviceIdType.MESH
F32 = jnp.float32
BF16 = jnp.bfloat16
I32 = jnp.int32

temper = 0.05
SCALE2 = 20.0 * 1.4426950408889634
LANES = 128
CAP = 8
WIDE = 4
UNROLL = 8
LOW = -3e38


def iota(shape, axis):
    return lax.broadcasted_iota(I32, shape, axis)


def to_row(col):
    n = col.shape[0]
    eye = iota((n, n), 0) == iota((n, n), 1)
    return jnp.sum(jnp.where(eye, col, jnp.zeros_like(col)), axis=0, keepdims=True)


def to_col(row):
    n = row.shape[1]
    eye = iota((n, n), 0) == iota((n, n), 1)
    return jnp.sum(jnp.where(eye, row, jnp.zeros_like(row)), axis=1, keepdims=True)


def pick(mask, values):
    return jnp.sum(jnp.where(mask, values, jnp.zeros_like(values)), axis=1, keepdims=True)


def step_kernel(
    G,
    R,
    NCH,
    cand_ref,
    omap_ref,
    q_ref,
    p_hbm,
    len_ref,
    teach_ref,
    w_ref,
    loss_ref,
    qgrad_ref,
    pgrad_ref,
    pt_v,
    p_f,
    p_v,
    q_all,
    c_v,
    x_s,
    y_r,
    t_r,
    v_r,
    g_r,
    wr,
    lr,
    meta_v,
    meta_s,
    m_v,
    att,
    u_v,
    slotr,
    loccol,
    sgq,
    sgl,
    qg_s,
    qg_r,
    acc,
    p_sem,
    meta_sem,
    y_send,
    y_recv,
    q_send,
    q_recv,
    t_send,
    t_recv,
    v_send,
    v_recv,
    g_send,
    g_recv,
    o_send,
    o_recv,
    w_send,
    w_recv,
    l_send,
    l_recv,
):
    me = lax.axis_index("grp")
    rep = lax.axis_index("rep")
    stored, token_len, dim = p_v.shape
    query_len = q_ref.shape[1]
    nslot = G * CAP

    def remote(src, dst, ssem, rsem, g, r):
        return pltpu.make_async_remote_copy(
            src_ref=src,
            dst_ref=dst,
            send_sem=ssem,
            recv_sem=rsem,
            device_id=(g, r),
            device_id_type=MESH,
        )

    def peers(body):
        def one(t, carry):
            body(lax.rem(me + t, G))
            return carry

        lax.fori_loop(1, G, one, 0)

    def reps(body):
        for t in range(1, R):
            body(lax.rem(rep + t, R))

    barrier = pltpu.get_barrier_semaphore()

    def greet(g):
        pl.semaphore_signal(barrier, inc=1, device_id=(g, rep), device_id_type=MESH)

    def greet_rep(r):
        pl.semaphore_signal(barrier, inc=1, device_id=(me, r), device_id_type=MESH)

    peers(greet)
    reps(greet_rep)
    p_copy = pltpu.make_async_copy(p_hbm, pt_v, p_sem)
    p_copy.start()

    c_v[:, 0:64] = cand_ref[0]
    c_v[:, 64:LANES] = cand_ref[1]
    omap = omap_ref[...]
    count = omap.shape[1]
    wanted = to_col(c_v[...])
    pos = pick(wanted == iota((LANES, count), 1), jnp.broadcast_to(omap, (LANES, count)))
    pos_row = to_row(pos)
    owner = pos_row >> 6
    row1 = (pos_row & 63) + 1
    x_s[:, 0, :] = jnp.where(owner == iota((G, LANES), 0), row1, 0).astype(F32)
    y_r[me] = x_s[me]
    q_all[pl.ds(2 * me, 2)] = q_ref[...]
    t_r[me, 0:1, 0:64] = teach_ref[0]
    t_r[me, 0:1, 64:LANES] = teach_ref[1]
    lane = iota((1, LANES), 1)
    t_r[me, 1:2, :] = jnp.where(lane < 64, w_ref[0, 0], w_ref[0, 1])

    pl.semaphore_wait(barrier, G - 1 + R - 1)

    def send_y(g):
        remote(x_s.at[g], y_r.at[me], y_send.at[g], y_recv.at[me], g, rep).start()

    def send_q(g):
        remote(
            q_ref, q_all.at[pl.ds(2 * me, 2)], q_send.at[g], q_recv.at[me], g, rep
        ).start()

    def send_t(g):
        remote(t_r.at[me], t_r.at[me], t_send.at[g], t_recv.at[me], g, rep).start()

    peers(send_y)
    peers(send_q)
    peers(send_t)

    def wait_y(g):
        remote(x_s.at[g], y_r.at[g], y_send.at[g], y_recv.at[g], g, rep).wait_recv()

    def wait_q(g):
        remote(
            q_ref, q_all.at[pl.ds(2 * g, 2)], q_send.at[g], q_recv.at[g], g, rep
        ).wait_recv()

    peers(wait_y)

    y = y_r[:, 0, :].astype(I32)
    have = y > 0
    lower = (iota((LANES, LANES), 0) < iota((LANES, LANES), 1)).astype(BF16)
    before = jnp.dot(have.astype(F32).astype(BF16), lower, preferred_element_type=F32).astype(I32)
    ylane = iota((G, LANES), 1)
    code = jnp.where(have, (y << 7) | ylane, 0)
    codes = [pick(have & (before == k), code) for k in range(CAP)]
    for k in range(CAP):
        rk = jnp.where(codes[k] > 0, codes[k] & 127, -1)
        slotr[k] = jnp.broadcast_to(rk, (G, LANES))
    ecode = jnp.concatenate(codes, axis=0)
    ew = ecode >> 7
    er = ecode & 127
    es = jnp.concatenate([iota((G, 1), 0)] * CAP, axis=0)
    ew_row = to_row(ew)
    used_row = ew_row > 0
    same = (ew == ew_row) & used_row
    rank = jnp.sum(
        jnp.where(same & (iota((nslot, nslot), 1) < iota((nslot, nslot), 0)), 1, 0),
        axis=1,
        keepdims=True,
    )
    rank_row = to_row(rank)
    starts = used_row & ((rank_row & (WIDE - 1)) == 0) & (ew_row < ew)
    base = jnp.sum(jnp.where(starts, 1, 0), axis=1, keepdims=True)
    loc = jnp.where(ew > 0, (base + (rank >> 2)) * WIDE + (rank & (WIDE - 1)), -1)
    loccol[...] = jnp.broadcast_to(loc, (nslot, LANES))
    packed = (ew << 12) | (es << 7) | er
    for b in range(WIDE):
        hit = loc == iota((nslot, LANES), 1) * WIDE + b
        meta_v[b : b + 1, :] = jnp.sum(jnp.where(hit, packed, 0), axis=0, keepdims=True)
    loc_row = to_row(loc)
    for h in range(nslot // LANES):
        meta_v[WIDE + h : WIDE + h + 1, :] = loc_row[:, h * LANES : (h + 1) * LANES]
    plane = iota((nslot, LANES), 1) + 1
    begin = (ew > 0) & ((rank & (WIDE - 1)) == 0)
    first = jnp.sum(jnp.where(begin & (ew < plane), 1, 0), axis=0, keepdims=True)
    held = jnp.sum(jnp.where(begin & (ew == plane), 1, 0), axis=0, keepdims=True)
    meta_v[6:7, :] = jnp.where(held > 0, first + 1, 0)
    meta_v[7:8, :] = jnp.zeros((1, LANES), I32)
    meta_copy = pltpu.make_async_copy(meta_v, meta_s, meta_sem)
    meta_copy.start()
    m_v[...] = jnp.zeros_like(m_v)
    meta_copy.wait()

    p_copy.wait()
    pitch = p_f.shape[0] // stored

    def spread(i, carry):
        for u in range(4):
            j = i * 4 + u
            p_f[pl.ds(j, stored, stride=pitch), :] = pt_v[j].astype(F32)
        return carry

    lax.fori_loop(0, token_len // 4, spread, 0)

    def settle(p, carry):
        p_v[p] = p_f[pl.ds(pl.multiple_of(p * pitch, 8), token_len), :].astype(BF16)
        return carry

    lax.fori_loop(0, stored, settle, 0)
    peers(wait_q)

    def wait_t(g):
        remote(t_r.at[g], t_r.at[g], t_send.at[g], t_recv.at[g], g, rep).wait_recv()

    peers(wait_t)

    wr[rep] = jnp.sum(t_r[:, 1, :], axis=0, keepdims=True)

    def send_w(r):
        remote(wr.at[rep], wr.at[rep], w_send.at[r], w_recv.at[rep], me, r).start()

    reps(send_w)

    def query_of(b, ch):
        return q_all[(meta_s[b, ch] >> 6) & (2 * G - 1)]

    def passage_of(ch):
        return jnp.maximum((meta_s[0, ch] >> 12) - 1, 0)

    token = iota((token_len, LANES), 0)

    def forward(ch):
        pid = passage_of(ch)
        queries = jnp.concatenate([query_of(b, ch) for b in range(WIDE)], axis=0)
        x = lax.dot_general(
            p_v[pid], queries, (((1,), (1,)), ((), ())), preferred_element_type=F32
        )
        x = jnp.where(token < len_ref[0, pid], x, -1e30)
        highest = jnp.max(x, axis=0, keepdims=True)
        powers = jnp.exp2((x - highest) * SCALE2)
        summed = jnp.sum(powers, axis=0, keepdims=True)
        att[ch] = (powers * (1.0 / summed)).astype(BF16)
        return highest + temper * jnp.log(summed)

    def forward_group(g, carry):
        rows = [forward(g * UNROLL + u) for u in range(UNROLL)]
        m_v[pl.ds(pl.multiple_of(g * UNROLL, UNROLL), UNROLL), :] = jnp.concatenate(rows, axis=0)
        return carry

    lax.fori_loop(0, NCH // UNROLL, forward_group, 0)

    matched = m_v[...]
    block = iota((LANES, LANES), 1) >> 5
    loc_cols = loccol[...]
    scores = jnp.zeros((nslot, 1), F32)
    for b in range(WIDE):
        row = to_row(pick(block == b, matched))
        hit = loc_cols == iota((nslot, LANES), 1) * WIDE + b
        scores += pick(hit, jnp.broadcast_to(row, (nslot, LANES)))
    slots = [slotr[k][:, 0:1] for k in range(CAP)]
    score = [scores[k * G : (k + 1) * G, :] for k in range(CAP)]
    belongs = [[(r >= 0) & (r < 64) for r in slots], [r >= 64 for r in slots]]
    spot = ylane - iota((G, LANES), 0)
    stats = jnp.zeros((1, LANES), F32)
    for h in (0, 1):
        top = jnp.full((G, 1), LOW, F32)
        for k in range(CAP):
            top = jnp.maximum(top, jnp.where(belongs[h][k], score[k], LOW))
        total = jnp.zeros((G, 1), F32)
        for k in range(CAP):
            total += jnp.where(belongs[h][k], jnp.exp(score[k] - top), 0.0)
        for col, shift in ((top, h * G), (total, 64 + h * G)):
            stats += jnp.sum(jnp.where(spot == shift, col, 0.0), axis=0, keepdims=True)
    v_r[me] = stats

    def send_v(g):
        remote(v_r.at[me], v_r.at[me], v_send.at[g], v_recv.at[me], g, rep).start()

    peers(send_v)

    def lift(ch):
        u = lax.dot_general(
            att[ch], p_v[passage_of(ch)], (((0,), (0,)), ((), ())), preferred_element_type=F32
        )
        u_v[pl.ds(ch * WIDE, WIDE)] = u.astype(BF16).reshape(WIDE, query_len, dim)

    def lift_group(g, carry):
        for u in range(UNROLL):
            lift(g * UNROLL + u)
        return carry

    lax.fori_loop(0, NCH // UNROLL, lift_group, 0)

    teacher = t_r[:, 0, :]
    half = ylane >> 6
    top = [jnp.max(jnp.where(half == h, teacher, LOW), axis=1, keepdims=True) for h in (0, 1)]
    shifted = teacher - jnp.where(half == 0, top[0], top[1])
    powers = jnp.exp(shifted)
    total = [pick(half == h, powers) for h in (0, 1)]
    log_teacher = shifted - jnp.log(jnp.where(half == 0, total[0], total[1]))
    weight = [pick(ylane == h * 64, t_r[:, 1, :]) for h in (0, 1)]

    def wait_v(g):
        remote(v_r.at[g], v_r.at[g], v_send.at[g], v_recv.at[g], g, rep).wait_recv()

    def wait_w(r):
        remote(wr.at[r], wr.at[r], w_send.at[r], w_recv.at[r], me, r).wait_recv()

    reps(wait_w)
    by_rep = jnp.sum(wr[...], axis=0)
    weight_sum = jnp.sum(jnp.where((lane & 63) == 0, by_rep, 0.0), axis=1, keepdims=True)
    peers(wait_v)

    stats = v_r[:, 0, :]
    top = jnp.max(stats, axis=0, keepdims=True)
    total = jnp.sum(pltpu.roll(stats, 64, 1) * jnp.exp(stats - top), axis=0, keepdims=True)
    log_total = top + jnp.log(total)
    log_totals = [pick(spot == h * G, jnp.broadcast_to(log_total, (G, LANES))) for h in (0, 1)]

    scale_all = 2.0 * G * R
    by_slot = []
    part = jnp.zeros((G, 1), F32)
    for k in range(CAP):
        late = belongs[1][k]
        valid = slots[k] >= 0
        log_t = pick(slotr[k] == ylane, log_teacher)
        log_s = score[k] - jnp.where(late, log_totals[1], log_totals[0])
        w = jnp.where(late, weight[1], weight[0])
        prob_t = jnp.exp(log_t)
        grad = scale_all * w / weight_sum * (jnp.exp(log_s) - prob_t)
        grad = jnp.where(valid, grad, 0.0)
        part += jnp.where(valid, w * (prob_t * (log_t - log_s)), 0.0)
        by_slot.append(grad)
        sgq[:, k, :] = jnp.broadcast_to(jnp.where(late, 0.0, grad), (G, LANES))
        sgq[:, CAP + k, :] = jnp.broadcast_to(jnp.where(late, grad, 0.0), (G, LANES))
    g_r[me] = jnp.broadcast_to(jnp.sum(part, axis=0, keepdims=True), (1, LANES))

    def send_g(g):
        remote(g_r.at[me], g_r.at[me], g_send.at[g], g_recv.at[me], g, rep).start()

    def wait_g(g):
        remote(g_r.at[g], g_r.at[g], g_send.at[g], g_recv.at[g], g, rep).wait_recv()

    def query_sum(s):
        scales = sgq[s]
        one = jnp.zeros((query_len, dim), F32)
        two = jnp.zeros((query_len, dim), F32)
        for k in range(CAP):
            e = k * G + s
            at = jnp.maximum(meta_s[WIDE + e // LANES, lax.rem(e, LANES)], 0)
            u = u_v[at].astype(F32)
            one += scales[k : k + 1, :] * u
            two += scales[CAP + k : CAP + k + 1, :] * u
        return one.astype(BF16), two.astype(BF16)

    def send_qg(t, carry):
        s = lax.rem(me + t, G)
        one, two = query_sum(s)
        qg_s[s, 0] = one
        qg_s[s, 1] = two
        remote(qg_s.at[s], qg_r.at[me], o_send.at[s], o_recv.at[me], s, rep).start()
        return carry

    lax.fori_loop(1, G, send_qg, 0)
    peers(send_g)
    one, two = query_sum(me)
    qg_r[me, 0] = one
    qg_r[me, 1] = two

    sg_row = to_row(jnp.concatenate(by_slot, axis=0))
    loc_rows = jnp.concatenate(
        [meta_v[WIDE + h : WIDE + h + 1, :] for h in range(nslot // LANES)], axis=1
    )
    for b in range(WIDE):
        hit = loc_rows == iota((LANES, nslot), 0) * WIDE + b
        col = pick(hit, jnp.broadcast_to(sg_row, (LANES, nslot)))
        sgl[:, b, :] = jnp.broadcast_to(col, (LANES, LANES))

    acc[...] = jnp.zeros_like(acc)

    def back(ch):
        scales = sgl[ch]
        scaled = jnp.concatenate(
            [
                (query_of(b, ch).astype(F32) * scales[b : b + 1, :]).astype(BF16)
                for b in range(WIDE)
            ],
            axis=0,
        )
        product = jnp.dot(att[ch], scaled, preferred_element_type=F32)
        follows = (meta_s[0, ch] >> 12) == (meta_s[0, ch + 1] >> 12)
        total = product + acc[...] * jnp.where(follows, 1.0, 0.0)
        acc[...] = total
        att[ch] = total.astype(BF16)

    def back_group(i, carry):
        g = NCH // UNROLL - 1 - i
        for u in range(UNROLL):
            back(g * UNROLL + UNROLL - 1 - u)
        return carry

    lax.fori_loop(0, NCH // UNROLL, back_group, 0)

    peers(wait_g)
    lr[rep] = jnp.sum(g_r[...], axis=0)

    def send_l(r):
        remote(lr.at[rep], lr.at[rep], l_send.at[r], l_recv.at[rep], me, r).start()

    reps(send_l)

    def place(p, carry):
        mark = meta_s[6, p]
        rows = att[jnp.maximum(mark - 1, 0)].astype(F32) * jnp.where(mark > 0, 1.0, 0.0)
        p_f[pl.ds(p, token_len, stride=stored), :] = rows
        return carry

    lax.fori_loop(0, stored, place, 0)

    def pack(i, carry):
        for u in range(4):
            j = i * 4 + u
            pgrad_ref[j] = p_f[pl.ds(pl.multiple_of(j * stored, stored), stored), :].astype(BF16)
        return carry

    lax.fori_loop(0, token_len // 4, pack, 0)

    def wait_l(r):
        remote(lr.at[r], lr.at[r], l_send.at[r], l_recv.at[r], me, r).wait_recv()

    reps(wait_l)
    loss_ref[...] = jnp.sum(lr[...], axis=0) / weight_sum

    def wait_o(g):
        remote(qg_s.at[g], qg_r.at[g], o_send.at[g], o_recv.at[g], g, rep).wait_recv()

    peers(wait_o)

    def add(o, carry):
        return carry + qg_r[o].astype(F32)

    qgrad_ref[...] = lax.fori_loop(0, G, add, jnp.zeros(qgrad_ref.shape, F32))

    def drain(g):
        remote(x_s.at[g], y_r.at[g], y_send.at[g], y_recv.at[g], g, rep).wait_send()
        remote(t_r.at[g], t_r.at[g], t_send.at[g], t_recv.at[g], g, rep).wait_send()
        remote(q_ref, q_all.at[pl.ds(2 * g, 2)], q_send.at[g], q_recv.at[g], g, rep).wait_send()
        remote(v_r.at[g], v_r.at[g], v_send.at[g], v_recv.at[g], g, rep).wait_send()
        remote(g_r.at[g], g_r.at[g], g_send.at[g], g_recv.at[g], g, rep).wait_send()
        remote(qg_s.at[g], qg_r.at[g], o_send.at[g], o_recv.at[g], g, rep).wait_send()

    def drain_rep(r):
        remote(wr.at[r], wr.at[r], w_send.at[r], w_recv.at[r], me, r).wait_send()
        remote(lr.at[r], lr.at[r], l_send.at[r], l_recv.at[r], me, r).wait_send()

    peers(drain)
    reps(drain_rep)


def on_device(G, R, queries, passages, lengths, cand_ids, owner_map, teacher, weights):
    query_local, _, query_len, dim = queries.shape
    stored, _, token_len, _ = passages.shape
    chunks = (G * CAP + (WIDE - 1) * stored) // WIDE
    NCH = -(-chunks // UNROLL) * UNROLL
    pitch = -(-token_len // 8) * 8
    vmem = pl.BlockSpec(memory_space=pltpu.VMEM)
    smem = pl.BlockSpec(memory_space=pltpu.SMEM)
    hbm = pl.BlockSpec(memory_space=pl.ANY)
    dma = pltpu.SemaphoreType.DMA
    shape = jax.ShapeDtypeStruct
    loss, qgrad, pgrad = pl.pallas_call(
        functools.partial(step_kernel, G, R, NCH),
        out_shape=(
            shape((1, LANES), F32),
            shape((query_local, query_len, dim), F32),
            pltpu.VMEM((token_len, stored, dim), BF16),
        ),
        in_specs=[vmem, vmem, vmem, hbm, smem, vmem, smem],
        out_specs=(vmem, vmem, vmem),
        scratch_shapes=[
            pltpu.VMEM((token_len, stored, dim), BF16),
            pltpu.VMEM((stored * pitch, dim), F32),
            pltpu.VMEM((stored, token_len, dim), BF16),
            pltpu.VMEM((query_local * G, query_len, dim), BF16),
            pltpu.VMEM((1, LANES), I32),
            pltpu.VMEM((G, 1, LANES), F32),
            pltpu.VMEM((G, 1, LANES), F32),
            pltpu.VMEM((G, 2, LANES), F32),
            pltpu.VMEM((G, 1, LANES), F32),
            pltpu.VMEM((G, 1, LANES), F32),
            pltpu.VMEM((R, 1, LANES), F32),
            pltpu.VMEM((R, 1, LANES), F32),
            pltpu.VMEM((8, LANES), I32),
            pltpu.SMEM((8, LANES), I32),
            pltpu.VMEM((LANES, LANES), F32),
            pltpu.VMEM((NCH, token_len, LANES), BF16),
            pltpu.VMEM((NCH * WIDE, query_len, dim), BF16),
            pltpu.VMEM((CAP, G, LANES), I32),
            pltpu.VMEM((G * CAP, LANES), I32),
            pltpu.VMEM((G, 2 * CAP, LANES), F32),
            pltpu.VMEM((LANES, WIDE, LANES), F32),
            pltpu.VMEM((G, query_local, query_len, dim), BF16),
            pltpu.VMEM((G, query_local, query_len, dim), BF16),
            pltpu.VMEM((token_len, dim), F32),
            dma,
            dma,
        ]
        + [dma((G,))] * 12
        + [dma((R,))] * 4,
        compiler_params=pltpu.CompilerParams(
            collective_id=0, has_side_effects=True, vmem_limit_bytes=56 * 1024 * 1024
        ),
    )(
        cand_ids,
        owner_map,
        queries.reshape(query_local, query_len, dim),
        jnp.transpose(passages[:, 0], (1, 0, 2)),
        lengths.reshape(1, stored),
        teacher,
        weights.reshape(1, query_local),
    )
    return loss[0, 0], qgrad[:, None], jnp.transpose(pgrad, (1, 0, 2))[:, None]


def solution(mesh):
    G, R = mesh.shape["grp"], mesh.shape["rep"]
    in_specs = (
        P("grp", "rep", None, None),
        P("grp", "rep", None, None),
        P("grp", "rep"),
        P("grp", "rep", None),
        P("rep", None),
        P("grp", "rep", None),
        P("grp", "rep"),
    )
    out_specs = (P(), P("grp", "rep", None, None), P("grp", "rep", None, None))
    return jax.shard_map(
        functools.partial(on_device, G, R),
        mesh=mesh,
        in_specs=in_specs,
        out_specs=out_specs,
        check_vma=False,
    )
```

```python
import functools

import jax
import jax.numpy as jnp
from jax import lax
from jax.experimental import pallas as pl
from jax.experimental.pallas import tpu as pltpu
from jax.sharding import PartitionSpec as P

MESH = pl.DeviceIdType.MESH
F32 = jnp.float32
BF16 = jnp.bfloat16
I32 = jnp.int32

temper = 0.05
SCALE2 = 20.0 * 1.4426950408889634
LANES = 128
CAP = 8
WIDE = 4
UNROLL = 8
LOW = -3e38
YN = 4


def iota(shape, axis):
    return lax.broadcasted_iota(I32, shape, axis)


def to_row(col):
    n = col.shape[0]
    eye = iota((n, n), 0) == iota((n, n), 1)
    return jnp.sum(jnp.where(eye, col, jnp.zeros_like(col)), axis=0, keepdims=True)


def to_col(row):
    n = row.shape[1]
    eye = iota((n, n), 0) == iota((n, n), 1)
    return jnp.sum(jnp.where(eye, row, jnp.zeros_like(row)), axis=1, keepdims=True)


def pick(mask, values):
    return jnp.sum(jnp.where(mask, values, jnp.zeros_like(values)), axis=1, keepdims=True)


def step_kernel(
    G,
    R,
    NCH,
    cand_ref,
    omap_ref,
    q_ref,
    p_hbm,
    len_ref,
    teach_ref,
    w_ref,
    loss_ref,
    qgrad_ref,
    pgrad_ref,
    pt_v,
    p_f,
    p_v,
    q_all,
    c_v,
    t_r,
    vz,
    vy,
    gz_r,
    gy_r,
    wr,
    lr,
    meta_v,
    meta_s,
    m_v,
    att,
    u_v,
    slotr,
    loccol,
    sgq,
    sgl,
    oy_s,
    oy_r,
    oz_s,
    oz_r,
    own,
    acc,
    p_sem,
    meta_sem,
    ty_send,
    ty_recv,
    qy_send,
    qy_recv,
    oy_send,
    oy_recv,
    tz_send,
    tz_recv,
    qz_send,
    qz_recv,
    oz_send,
    oz_recv,
    vz_send,
    vz_recv,
    gz_send,
    gz_recv,
    vy_send,
    vy_recv,
    gy_send,
    gy_recv,
    w_send,
    w_recv,
    l_send,
    l_recv,
):
    me = lax.axis_index("grp")
    rep = lax.axis_index("rep")
    ZN = G // YN
    z, y = me // YN, lax.rem(me, YN)
    stored, token_len, dim = p_v.shape
    query_len = q_ref.shape[1]
    nslot = G * CAP

    def remote(src, dst, ssem, rsem, g, r):
        return pltpu.make_async_remote_copy(
            src_ref=src,
            dst_ref=dst,
            send_sem=ssem,
            recv_sem=rsem,
            device_id=(g, r),
            device_id_type=MESH,
        )

    def near_z(t):
        odd = lax.rem(t, 2)
        return lax.rem(z + odd * ((t + 1) // 2) + (1 - odd) * (ZN - t // 2), ZN)

    def over_z(body, far=False):
        def one(t, carry):
            body(near_z(ZN - t if far else t))
            return carry

        lax.fori_loop(1, ZN, one, 0)

    def over_y(body):
        for t in range(1, YN):
            body(lax.rem(y + t, YN))

    def over_rep(body):
        for t in range(1, R):
            body(lax.rem(rep + t, R))

    barrier = pltpu.get_barrier_semaphore()

    def greet(g, r):
        pl.semaphore_signal(barrier, inc=1, device_id=(g, r), device_id_type=MESH)

    over_z(lambda zz: greet(zz * YN + y, rep))
    over_y(lambda yy: greet(z * YN + yy, rep))
    over_rep(lambda rr: greet(me, rr))
    p_copy = pltpu.make_async_copy(p_hbm, pt_v, p_sem)
    p_copy.start()

    c_v[:, 0:64] = cand_ref[0]
    c_v[:, 64:LANES] = cand_ref[1]
    omap = omap_ref[...]
    count = omap.shape[1]
    wanted = to_col(c_v[...])
    pos = pick(wanted == iota((LANES, count), 1), jnp.broadcast_to(omap, (LANES, count)))
    lane = iota((1, LANES), 1)
    t_r[me, 0:1, 0:64] = teach_ref[0]
    t_r[me, 0:1, 64:LANES] = teach_ref[1]
    t_r[me, 1:2, :] = jnp.where(lane < 64, w_ref[0, 0], w_ref[0, 1])
    t_r[me, 2:3, :] = to_row(pos).astype(F32)
    q_all[pl.ds(2 * me, 2)] = q_ref[...]

    pl.semaphore_wait(barrier, ZN - 1 + YN - 1 + R - 1)

    def t_z(to, src):
        g = src * YN + y
        return remote(t_r.at[g], t_r.at[g], tz_send.at[to], tz_recv.at[src], to * YN + y, rep)

    def q_z(to, src):
        rows = q_all.at[pl.ds(2 * (src * YN + y), 2)]
        return remote(rows, rows, qz_send.at[to], qz_recv.at[src], to * YN + y, rep)

    def t_y(to, g):
        ssem = ty_send.at[g // YN * YN + to]
        return remote(t_r.at[g], t_r.at[g], ssem, ty_recv.at[g], z * YN + to, rep)

    def q_y(to, g):
        rows = q_all.at[pl.ds(2 * g, 2)]
        ssem = qy_send.at[g // YN * YN + to]
        return remote(rows, rows, ssem, qy_recv.at[g], z * YN + to, rep)

    over_z(lambda zz: t_z(zz, z).start())
    over_y(lambda yy: t_y(yy, me).start())
    over_z(lambda zz: q_z(zz, z).start())
    over_y(lambda yy: q_y(yy, me).start())

    def pass_t(zz):
        t_z(z, zz).wait_recv()
        over_y(lambda yy: t_y(yy, zz * YN + y).start())

    def pass_q(zz):
        q_z(z, zz).wait_recv()
        over_y(lambda yy: q_y(yy, zz * YN + y).start())

    over_z(pass_t)
    over_z(pass_q)

    p_copy.wait()
    pitch = p_f.shape[0] // stored

    def spread(i, carry):
        for u in range(4):
            j = i * 4 + u
            p_f[pl.ds(j, stored, stride=pitch), :] = pt_v[j].astype(F32)
        return carry

    lax.fori_loop(0, token_len // 4, spread, 0)

    def settle(p, carry):
        p_v[p] = p_f[pl.ds(pl.multiple_of(p * pitch, 8), token_len), :].astype(BF16)
        return carry

    lax.fori_loop(0, stored, settle, 0)

    def all_z(body):
        def one(zz, carry):
            body(zz)
            return carry

        lax.fori_loop(0, ZN, one, 0)

    all_z(lambda zz: over_y(lambda yy: t_y(y, zz * YN + yy).wait_recv()))

    wr[rep] = jnp.sum(t_r[:, 1, :], axis=0, keepdims=True)

    def w_rep(to, src):
        return remote(wr.at[src], wr.at[src], w_send.at[to], w_recv.at[src], me, to)

    over_rep(lambda rr: w_rep(rr, rep).start())

    spots = t_r[:, 2, :].astype(I32)
    have = (spots >> 6) == me
    lower = (iota((LANES, LANES), 0) < iota((LANES, LANES), 1)).astype(BF16)
    before = jnp.dot(have.astype(F32).astype(BF16), lower, preferred_element_type=F32).astype(I32)
    ylane = iota((G, LANES), 1)
    code = jnp.where(have, (((spots & 63) + 1) << 7) | ylane, 0)
    codes = [pick(have & (before == k), code) for k in range(CAP)]
    for k in range(CAP):
        rk = jnp.where(codes[k] > 0, codes[k] & 127, -1)
        slotr[k] = jnp.broadcast_to(rk, (G, LANES))
    ecode = jnp.concatenate(codes, axis=0)
    ew = ecode >> 7
    er = ecode & 127
    es = jnp.concatenate([iota((G, 1), 0)] * CAP, axis=0)
    ew_row = to_row(ew)
    used_row = ew_row > 0
    same = (ew == ew_row) & used_row
    rank = jnp.sum(
        jnp.where(same & (iota((nslot, nslot), 1) < iota((nslot, nslot), 0)), 1, 0),
        axis=1,
        keepdims=True,
    )
    rank_row = to_row(rank)
    starts = used_row & ((rank_row & (WIDE - 1)) == 0) & (ew_row < ew)
    base = jnp.sum(jnp.where(starts, 1, 0), axis=1, keepdims=True)
    loc = jnp.where(ew > 0, (base + (rank >> 2)) * WIDE + (rank & (WIDE - 1)), -1)
    loccol[...] = jnp.broadcast_to(loc, (nslot, LANES))
    packed = (ew << 12) | (es << 7) | er
    for b in range(WIDE):
        hit = loc == iota((nslot, LANES), 1) * WIDE + b
        meta_v[b : b + 1, :] = jnp.sum(jnp.where(hit, packed, 0), axis=0, keepdims=True)
    loc_row = to_row(loc)
    for h in range(nslot // LANES):
        meta_v[WIDE + h : WIDE + h + 1, :] = loc_row[:, h * LANES : (h + 1) * LANES]
    plane = iota((nslot, LANES), 1) + 1
    begin = (ew > 0) & ((rank & (WIDE - 1)) == 0)
    first = jnp.sum(jnp.where(begin & (ew < plane), 1, 0), axis=0, keepdims=True)
    held = jnp.sum(jnp.where(begin & (ew == plane), 1, 0), axis=0, keepdims=True)
    meta_v[6:7, :] = jnp.where(held > 0, first + 1, 0)
    meta_v[7:8, :] = jnp.zeros((1, LANES), I32)
    meta_copy = pltpu.make_async_copy(meta_v, meta_s, meta_sem)
    meta_copy.start()
    m_v[...] = jnp.zeros_like(m_v)
    meta_copy.wait()

    all_z(lambda zz: over_y(lambda yy: q_y(y, zz * YN + yy).wait_recv()))

    def query_of(b, ch):
        return q_all[(meta_s[b, ch] >> 6) & (2 * G - 1)]

    def passage_of(ch):
        return jnp.maximum((meta_s[0, ch] >> 12) - 1, 0)

    token = iota((token_len, LANES), 0)

    def forward(ch):
        pid = passage_of(ch)
        queries = jnp.concatenate([query_of(b, ch) for b in range(WIDE)], axis=0)
        x = lax.dot_general(
            p_v[pid], queries, (((1,), (1,)), ((), ())), preferred_element_type=F32
        )
        x = jnp.where(token < len_ref[0, pid], x, -1e30)
        highest = jnp.max(x, axis=0, keepdims=True)
        powers = jnp.exp2((x - highest) * SCALE2)
        summed = jnp.sum(powers, axis=0, keepdims=True)
        att[ch] = (powers * (1.0 / summed)).astype(BF16)
        return highest + temper * jnp.log(summed)

    def forward_group(g, carry):
        rows = [forward(g * UNROLL + u) for u in range(UNROLL)]
        m_v[pl.ds(pl.multiple_of(g * UNROLL, UNROLL), UNROLL), :] = jnp.concatenate(rows, axis=0)
        return carry

    lax.fori_loop(0, NCH // UNROLL, forward_group, 0)

    matched = m_v[...]
    block = iota((LANES, LANES), 1) >> 5
    loc_cols = loccol[...]
    scores = jnp.zeros((nslot, 1), F32)
    for b in range(WIDE):
        row = to_row(pick(block == b, matched))
        hit = loc_cols == iota((nslot, LANES), 1) * WIDE + b
        scores += pick(hit, jnp.broadcast_to(row, (nslot, LANES)))
    slots = [slotr[k][:, 0:1] for k in range(CAP)]
    score = [scores[k * G : (k + 1) * G, :] for k in range(CAP)]
    belongs = [[(r >= 0) & (r < 64) for r in slots], [r >= 64 for r in slots]]
    spot = ylane - iota((G, LANES), 0)
    stats = jnp.zeros((1, LANES), F32)
    for h in (0, 1):
        top = jnp.full((G, 1), LOW, F32)
        for k in range(CAP):
            top = jnp.maximum(top, jnp.where(belongs[h][k], score[k], LOW))
        total = jnp.zeros((G, 1), F32)
        for k in range(CAP):
            total += jnp.where(belongs[h][k], jnp.exp(score[k] - top), 0.0)
        for col, shift in ((top, h * G), (total, 64 + h * G)):
            stats += jnp.sum(jnp.where(spot == shift, col, 0.0), axis=0, keepdims=True)
    vz[z] = stats

    def v_z(to, src):
        return remote(vz.at[src], vz.at[src], vz_send.at[to], vz_recv.at[src], to * YN + y, rep)

    def v_y(to, src):
        return remote(vy.at[src], vy.at[src], vy_send.at[to], vy_recv.at[src], z * YN + to, rep)

    over_z(lambda zz: v_z(zz, z).start())

    def lift(ch):
        u = lax.dot_general(
            att[ch], p_v[passage_of(ch)], (((0,), (0,)), ((), ())), preferred_element_type=F32
        )
        u_v[pl.ds(ch * WIDE, WIDE)] = u.astype(BF16).reshape(WIDE, query_len, dim)

    def lift_group(g, carry):
        for u in range(UNROLL):
            lift(g * UNROLL + u)
        return carry

    groups = NCH // UNROLL
    lax.fori_loop(0, groups // 2, lift_group, 0)

    def combine(stats):
        top = jnp.max(stats, axis=0, keepdims=True)
        total = jnp.sum(pltpu.roll(stats, 64, 1) * jnp.exp(stats - top), axis=0, keepdims=True)
        return top, total

    over_z(lambda zz: v_z(z, zz).wait_recv())
    top, total = combine(vz[:, 0, :])
    vy[y] = jnp.where(lane < 64, top, pltpu.roll(total, 64, 1))
    over_y(lambda yy: v_y(yy, y).start())
    lax.fori_loop(groups // 2, groups, lift_group, 0)

    teacher = t_r[:, 0, :]
    half = ylane >> 6
    top = [jnp.max(jnp.where(half == h, teacher, LOW), axis=1, keepdims=True) for h in (0, 1)]
    shifted = teacher - jnp.where(half == 0, top[0], top[1])
    powers = jnp.exp(shifted)
    total = [pick(half == h, powers) for h in (0, 1)]
    log_teacher = shifted - jnp.log(jnp.where(half == 0, total[0], total[1]))
    weight = [pick(ylane == h * 64, t_r[:, 1, :]) for h in (0, 1)]

    over_rep(lambda rr: w_rep(rep, rr).wait_recv())
    by_rep = jnp.sum(wr[...], axis=0)
    weight_sum = jnp.sum(jnp.where((lane & 63) == 0, by_rep, 0.0), axis=1, keepdims=True)
    over_y(lambda yy: v_y(y, yy).wait_recv())
    top, total = combine(vy[:, 0, :])
    log_total = top + jnp.log(total)
    log_totals = [pick(spot == h * G, jnp.broadcast_to(log_total, (G, LANES))) for h in (0, 1)]

    scale_all = 2.0 * G * R
    by_slot = []
    part = jnp.zeros((G, 1), F32)
    for k in range(CAP):
        late = belongs[1][k]
        valid = slots[k] >= 0
        log_t = pick(slotr[k] == ylane, log_teacher)
        log_s = score[k] - jnp.where(late, log_totals[1], log_totals[0])
        w = jnp.where(late, weight[1], weight[0])
        prob_t = jnp.exp(log_t)
        grad = scale_all * w / weight_sum * (jnp.exp(log_s) - prob_t)
        grad = jnp.where(valid, grad, 0.0)
        part += jnp.where(valid, w * (prob_t * (log_t - log_s)), 0.0)
        by_slot.append(grad)
        sgq[:, k, :] = jnp.broadcast_to(jnp.where(late, 0.0, grad), (G, LANES))
        sgq[:, CAP + k, :] = jnp.broadcast_to(jnp.where(late, grad, 0.0), (G, LANES))
    gz_r[z] = jnp.broadcast_to(jnp.sum(part, axis=0, keepdims=True), (1, LANES))

    def g_z(to, src):
        return remote(gz_r.at[src], gz_r.at[src], gz_send.at[to], gz_recv.at[src], to * YN + y, rep)

    def g_y(to, src):
        return remote(gy_r.at[src], gy_r.at[src], gy_send.at[to], gy_recv.at[src], z * YN + to, rep)

    def l_rep(to, src):
        return remote(lr.at[src], lr.at[src], l_send.at[to], l_recv.at[src], me, to)

    over_z(lambda zz: g_z(zz, z).start())

    def query_sum(s):
        scales = sgq[s]
        one = jnp.zeros((query_len, dim), F32)
        two = jnp.zeros((query_len, dim), F32)
        for k in range(CAP):
            e = k * G + s
            at = jnp.maximum(meta_s[WIDE + e // LANES, lax.rem(e, LANES)], 0)
            u = u_v[at].astype(F32)
            one += scales[k : k + 1, :] * u
            two += scales[CAP + k : CAP + k + 1, :] * u
        return one, two

    def o_y(to, zz, src):
        ssem, rsem = oy_send.at[zz * YN + to], oy_recv.at[zz * YN + src]
        dst = oy_r.at[zz * YN + src]
        return remote(oy_s.at[zz * YN + to], dst, ssem, rsem, z * YN + to, rep)

    def o_z(to, src):
        return remote(oz_s.at[to], oz_r.at[src], oz_send.at[to], oz_recv.at[src], to * YN + y, rep)

    def send_sums(zz):
        def one_way(yy):
            one, two = query_sum(zz * YN + yy)
            oy_s[zz * YN + yy, 0] = one.astype(BF16)
            oy_s[zz * YN + yy, 1] = two.astype(BF16)
            o_y(yy, zz, y).start()

        over_y(one_way)

    over_z(send_sums, far=True)
    send_sums(z)

    def keep_sums(zz):
        one, two = query_sum(zz * YN + y)
        own[zz, 0] = one
        own[zz, 1] = two

    all_z(keep_sums)

    sg_row = to_row(jnp.concatenate(by_slot, axis=0))
    loc_rows = jnp.concatenate(
        [meta_v[WIDE + h : WIDE + h + 1, :] for h in range(nslot // LANES)], axis=1
    )
    for b in range(WIDE):
        hit = loc_rows == iota((LANES, nslot), 0) * WIDE + b
        col = pick(hit, jnp.broadcast_to(sg_row, (LANES, nslot)))
        sgl[:, b, :] = jnp.broadcast_to(col, (LANES, LANES))

    acc[...] = jnp.zeros_like(acc)

    def back(ch):
        scales = sgl[ch]
        scaled = jnp.concatenate(
            [
                (query_of(b, ch).astype(F32) * scales[b : b + 1, :]).astype(BF16)
                for b in range(WIDE)
            ],
            axis=0,
        )
        product = jnp.dot(att[ch], scaled, preferred_element_type=F32)
        follows = (meta_s[0, ch] >> 12) == (meta_s[0, ch + 1] >> 12)
        total = product + acc[...] * jnp.where(follows, 1.0, 0.0)
        acc[...] = total
        att[ch] = total.astype(BF16)

    def back_group(i, carry):
        g = groups - 1 - i
        for u in range(UNROLL):
            back(g * UNROLL + UNROLL - 1 - u)
        return carry

    lax.fori_loop(0, groups, back_group, 0)

    over_z(lambda zz: g_z(z, zz).wait_recv())
    gy_r[y] = jnp.sum(gz_r[...], axis=0)
    over_y(lambda yy: g_y(yy, y).start())

    def line_sum(zz):
        total = own[zz]

        for t in range(1, YN):
            yy = lax.rem(y + t, YN)
            o_y(y, zz, yy).wait_recv()
            total += oy_r[zz * YN + yy].astype(F32)
        return total

    def send_line(zz):
        oz_s[zz] = line_sum(zz).astype(BF16)
        o_z(zz, z).start()

    over_z(send_line, far=True)
    own[z] = line_sum(z)

    over_y(lambda yy: g_y(y, yy).wait_recv())
    lr[rep] = jnp.sum(gy_r[...], axis=0)
    over_rep(lambda rr: l_rep(rr, rep).start())

    def place(p, carry):
        mark = meta_s[6, p]
        rows = att[jnp.maximum(mark - 1, 0)].astype(F32) * jnp.where(mark > 0, 1.0, 0.0)
        p_f[pl.ds(p, token_len, stride=stored), :] = rows
        return carry

    lax.fori_loop(0, stored, place, 0)

    def pack(i, carry):
        for u in range(4):
            j = i * 4 + u
            pgrad_ref[j] = p_f[pl.ds(pl.multiple_of(j * stored, stored), stored), :].astype(BF16)
        return carry

    lax.fori_loop(0, token_len // 4, pack, 0)

    over_rep(lambda rr: l_rep(rep, rr).wait_recv())
    loss_ref[...] = jnp.sum(lr[...], axis=0) / weight_sum

    qgrad_ref[...] = own[z]

    def add(zz):
        o_z(z, zz).wait_recv()
        qgrad_ref[...] += oz_r[zz].astype(F32)

    over_z(add)

    def drain_z(zz):
        for copy in (t_z, q_z, v_z, g_z, o_z):
            copy(zz, z).wait_send()

    def drain_y(zz, yy):
        t_y(yy, zz * YN + y).wait_send()
        q_y(yy, zz * YN + y).wait_send()
        o_y(yy, zz, y).wait_send()

    over_z(drain_z)
    all_z(lambda zz: over_y(lambda yy: drain_y(zz, yy)))
    over_y(lambda yy: v_y(yy, y).wait_send())
    over_y(lambda yy: g_y(yy, y).wait_send())
    over_rep(lambda rr: w_rep(rr, rep).wait_send())
    over_rep(lambda rr: l_rep(rr, rep).wait_send())


def on_device(G, R, queries, passages, lengths, cand_ids, owner_map, teacher, weights):
    query_local, _, query_len, dim = queries.shape
    stored, _, token_len, _ = passages.shape
    chunks = (G * CAP + (WIDE - 1) * stored) // WIDE
    NCH = -(-chunks // UNROLL) * UNROLL
    pitch = -(-token_len // 8) * 8
    ZN = G // YN
    vmem = pl.BlockSpec(memory_space=pltpu.VMEM)
    smem = pl.BlockSpec(memory_space=pltpu.SMEM)
    hbm = pl.BlockSpec(memory_space=pl.ANY)
    dma = pltpu.SemaphoreType.DMA
    shape = jax.ShapeDtypeStruct
    loss, qgrad, pgrad = pl.pallas_call(
        functools.partial(step_kernel, G, R, NCH),
        out_shape=(
            shape((1, LANES), F32),
            shape((query_local, query_len, dim), F32),
            pltpu.VMEM((token_len, stored, dim), BF16),
        ),
        in_specs=[vmem, vmem, vmem, hbm, smem, vmem, smem],
        out_specs=(vmem, vmem, vmem),
        scratch_shapes=[
            pltpu.VMEM((token_len, stored, dim), BF16),
            pltpu.VMEM((stored * pitch, dim), F32),
            pltpu.VMEM((stored, token_len, dim), BF16),
            pltpu.VMEM((query_local * G, query_len, dim), BF16),
            pltpu.VMEM((1, LANES), I32),
            pltpu.VMEM((G, 3, LANES), F32),
            pltpu.VMEM((ZN, 1, LANES), F32),
            pltpu.VMEM((YN, 1, LANES), F32),
            pltpu.VMEM((ZN, 1, LANES), F32),
            pltpu.VMEM((YN, 1, LANES), F32),
            pltpu.VMEM((R, 1, LANES), F32),
            pltpu.VMEM((R, 1, LANES), F32),
            pltpu.VMEM((8, LANES), I32),
            pltpu.SMEM((8, LANES), I32),
            pltpu.VMEM((LANES, LANES), F32),
            pltpu.VMEM((NCH, token_len, LANES), BF16),
            pltpu.VMEM((NCH * WIDE, query_len, dim), BF16),
            pltpu.VMEM((CAP, G, LANES), I32),
            pltpu.VMEM((G * CAP, LANES), I32),
            pltpu.VMEM((G, 2 * CAP, LANES), F32),
            pltpu.VMEM((LANES, WIDE, LANES), F32),
            pltpu.VMEM((G, query_local, query_len, dim), BF16),
            pltpu.VMEM((G, query_local, query_len, dim), BF16),
            pltpu.VMEM((ZN, query_local, query_len, dim), BF16),
            pltpu.VMEM((ZN, query_local, query_len, dim), BF16),
            pltpu.VMEM((ZN, query_local, query_len, dim), F32),
            pltpu.VMEM((token_len, dim), F32),
            dma,
            dma,
        ]
        + [dma((G,))] * 6
        + [dma((ZN,))] * 10
        + [dma((YN,))] * 4
        + [dma((R,))] * 4,
        compiler_params=pltpu.CompilerParams(
            collective_id=0, has_side_effects=True, vmem_limit_bytes=56 * 1024 * 1024
        ),
    )(
        cand_ids,
        owner_map,
        queries.reshape(query_local, query_len, dim),
        jnp.transpose(passages[:, 0], (1, 0, 2)),
        lengths.reshape(1, stored),
        teacher,
        weights.reshape(1, query_local),
    )
    return loss[0, 0], qgrad[:, None], jnp.transpose(pgrad, (1, 0, 2))[:, None]


def solution(mesh):
    G, R = mesh.shape["grp"], mesh.shape["rep"]
    in_specs = (
        P("grp", "rep", None, None),
        P("grp", "rep", None, None),
        P("grp", "rep"),
        P("grp", "rep", None),
        P("rep", None),
        P("grp", "rep", None),
        P("grp", "rep"),
    )
    out_specs = (P(), P("grp", "rep", None, None), P("grp", "rep", None, None))
    return jax.shard_map(
        functools.partial(on_device, G, R),
        mesh=mesh,
        in_specs=in_specs,
        out_specs=out_specs,
        check_vma=False,
    )
```

```python
import functools

import jax
import jax.numpy as jnp
from jax import lax
from jax.experimental import pallas as pl
from jax.experimental.pallas import tpu as pltpu
from jax.sharding import PartitionSpec as P

MESH = pl.DeviceIdType.MESH
F32 = jnp.float32
BF16 = jnp.bfloat16
I32 = jnp.int32

temper = 0.05
SCALE2 = 20.0 * 1.4426950408889634
LANES = 128
CAP = 8
WIDE = 4
UNROLL = 8
LOW = -3e38
YN = 4


def iota(shape, axis):
    return lax.broadcasted_iota(I32, shape, axis)


def to_row(col):
    n = col.shape[0]
    eye = iota((n, n), 0) == iota((n, n), 1)
    return jnp.sum(jnp.where(eye, col, jnp.zeros_like(col)), axis=0, keepdims=True)


def to_col(row):
    n = row.shape[1]
    eye = iota((n, n), 0) == iota((n, n), 1)
    return jnp.sum(jnp.where(eye, row, jnp.zeros_like(row)), axis=1, keepdims=True)


def pick(mask, values):
    return jnp.sum(jnp.where(mask, values, jnp.zeros_like(values)), axis=1, keepdims=True)


def step_kernel(
    G,
    R,
    NCH,
    cand_ref,
    omap_ref,
    q_ref,
    p_hbm,
    len_ref,
    teach_ref,
    w_ref,
    loss_ref,
    qgrad_ref,
    pgrad_ref,
    pt_v,
    p_f,
    p_v,
    q_all,
    c_v,
    t_r,
    v_r,
    gz_r,
    gy_r,
    wr,
    lr,
    meta_v,
    meta_s,
    m_v,
    att,
    u_v,
    slotr,
    loccol,
    sgq,
    sgl,
    oy_s,
    oy_r,
    oz_s,
    oz_r,
    own,
    acc,
    p_sem,
    meta_sem,
    ty_send,
    ty_recv,
    qy_send,
    qy_recv,
    oy_send,
    oy_recv,
    v_send,
    v_recv,
    tz_send,
    tz_recv,
    qz_send,
    qz_recv,
    oz_send,
    oz_recv,
    gz_send,
    gz_recv,
    gy_send,
    gy_recv,
    w_send,
    w_recv,
    l_send,
    l_recv,
):
    me = lax.axis_index("grp")
    rep = lax.axis_index("rep")
    ZN = G // YN
    z, y = me // YN, lax.rem(me, YN)
    stored, token_len, dim = p_v.shape
    query_len = q_ref.shape[1]
    nslot = G * CAP

    def remote(src, dst, ssem, rsem, g, r):
        return pltpu.make_async_remote_copy(
            src_ref=src,
            dst_ref=dst,
            send_sem=ssem,
            recv_sem=rsem,
            device_id=(g, r),
            device_id_type=MESH,
        )

    def near_z(t):
        odd = lax.rem(t, 2)
        return lax.rem(z + odd * ((t + 1) // 2) + (1 - odd) * (ZN - t // 2), ZN)

    def over_z(body, far=False):
        def one(t, carry):
            body(near_z(ZN - t if far else t))
            return carry

        lax.fori_loop(1, ZN, one, 0)

    def over_y(body):
        for t in range(1, YN):
            body(lax.rem(y + t, YN))

    def over_rep(body):
        for t in range(1, R):
            body(lax.rem(rep + t, R))

    barrier = pltpu.get_barrier_semaphore()

    def greet(g, r):
        pl.semaphore_signal(barrier, inc=1, device_id=(g, r), device_id_type=MESH)

    over_z(lambda zz: greet(zz * YN + y, rep))
    over_y(lambda yy: greet(z * YN + yy, rep))
    over_rep(lambda rr: greet(me, rr))
    p_copy = pltpu.make_async_copy(p_hbm, pt_v, p_sem)
    p_copy.start()

    c_v[:, 0:64] = cand_ref[0]
    c_v[:, 64:LANES] = cand_ref[1]
    omap = omap_ref[...]
    count = omap.shape[1]
    wanted = to_col(c_v[...])
    pos = pick(wanted == iota((LANES, count), 1), jnp.broadcast_to(omap, (LANES, count)))
    lane = iota((1, LANES), 1)
    t_r[me, 0:1, 0:64] = teach_ref[0]
    t_r[me, 0:1, 64:LANES] = teach_ref[1]
    t_r[me, 1:2, :] = jnp.where(lane < 64, w_ref[0, 0], w_ref[0, 1])
    t_r[me, 2:3, :] = to_row(pos).astype(F32)
    q_all[pl.ds(2 * me, 2)] = q_ref[...]

    pl.semaphore_wait(barrier, ZN - 1 + YN - 1 + R - 1)

    def t_z(to, src):
        g = src * YN + y
        return remote(t_r.at[g], t_r.at[g], tz_send.at[to], tz_recv.at[src], to * YN + y, rep)

    def q_z(to, src):
        rows = q_all.at[pl.ds(2 * (src * YN + y), 2)]
        return remote(rows, rows, qz_send.at[to], qz_recv.at[src], to * YN + y, rep)

    def t_y(to, g):
        ssem = ty_send.at[g // YN * YN + to]
        return remote(t_r.at[g], t_r.at[g], ssem, ty_recv.at[g], z * YN + to, rep)

    def q_y(to, g):
        rows = q_all.at[pl.ds(2 * g, 2)]
        ssem = qy_send.at[g // YN * YN + to]
        return remote(rows, rows, ssem, qy_recv.at[g], z * YN + to, rep)

    over_z(lambda zz: t_z(zz, z).start())
    over_y(lambda yy: t_y(yy, me).start())
    over_z(lambda zz: q_z(zz, z).start())
    over_y(lambda yy: q_y(yy, me).start())

    def pass_t(zz):
        t_z(z, zz).wait_recv()
        over_y(lambda yy: t_y(yy, zz * YN + y).start())

    def pass_q(zz):
        q_z(z, zz).wait_recv()
        over_y(lambda yy: q_y(yy, zz * YN + y).start())

    pass_t(near_z(1))

    def pass_on(t, carry):
        pass_t(near_z(t + 1))
        pass_q(near_z(t))
        return carry

    lax.fori_loop(1, ZN - 1, pass_on, 0)
    pass_q(near_z(ZN - 1))

    p_copy.wait()
    pitch = p_f.shape[0] // stored

    def spread(i, carry):
        for u in range(4):
            j = i * 4 + u
            p_f[pl.ds(j, stored, stride=pitch), :] = pt_v[j].astype(F32)
        return carry

    lax.fori_loop(0, token_len // 4, spread, 0)

    def settle(p, carry):
        p_v[p] = p_f[pl.ds(pl.multiple_of(p * pitch, 8), token_len), :].astype(BF16)
        return carry

    lax.fori_loop(0, stored, settle, 0)

    def all_z(body):
        def one(zz, carry):
            body(zz)
            return carry

        lax.fori_loop(0, ZN, one, 0)

    all_z(lambda zz: over_y(lambda yy: t_y(y, zz * YN + yy).wait_recv()))

    wr[rep] = jnp.sum(t_r[:, 1, :], axis=0, keepdims=True)

    def w_rep(to, src):
        return remote(wr.at[src], wr.at[src], w_send.at[to], w_recv.at[src], me, to)

    over_rep(lambda rr: w_rep(rr, rep).start())

    spots = t_r[:, 2, :].astype(I32)
    have = (spots >> 6) == me
    lower = (iota((LANES, LANES), 0) < iota((LANES, LANES), 1)).astype(BF16)
    before = jnp.dot(have.astype(F32).astype(BF16), lower, preferred_element_type=F32).astype(I32)
    ylane = iota((G, LANES), 1)
    code = jnp.where(have, (((spots & 63) + 1) << 7) | ylane, 0)
    codes = [pick(have & (before == k), code) for k in range(CAP)]
    for k in range(CAP):
        rk = jnp.where(codes[k] > 0, codes[k] & 127, -1)
        slotr[k] = jnp.broadcast_to(rk, (G, LANES))
    ecode = jnp.concatenate(codes, axis=0)
    ew = ecode >> 7
    er = ecode & 127
    es = jnp.concatenate([iota((G, 1), 0)] * CAP, axis=0)
    ew_row = to_row(ew)
    used_row = ew_row > 0
    same = (ew == ew_row) & used_row
    rank = jnp.sum(
        jnp.where(same & (iota((nslot, nslot), 1) < iota((nslot, nslot), 0)), 1, 0),
        axis=1,
        keepdims=True,
    )
    rank_row = to_row(rank)
    starts = used_row & ((rank_row & (WIDE - 1)) == 0) & (ew_row < ew)
    base = jnp.sum(jnp.where(starts, 1, 0), axis=1, keepdims=True)
    loc = jnp.where(ew > 0, (base + (rank >> 2)) * WIDE + (rank & (WIDE - 1)), -1)
    loccol[...] = jnp.broadcast_to(loc, (nslot, LANES))
    packed = (ew << 12) | (es << 7) | er
    for b in range(WIDE):
        hit = loc == iota((nslot, LANES), 1) * WIDE + b
        meta_v[b : b + 1, :] = jnp.sum(jnp.where(hit, packed, 0), axis=0, keepdims=True)
    loc_row = to_row(loc)
    for h in range(nslot // LANES):
        meta_v[WIDE + h : WIDE + h + 1, :] = loc_row[:, h * LANES : (h + 1) * LANES]
    plane = iota((nslot, LANES), 1) + 1
    begin = (ew > 0) & ((rank & (WIDE - 1)) == 0)
    first = jnp.sum(jnp.where(begin & (ew < plane), 1, 0), axis=0, keepdims=True)
    held = jnp.sum(jnp.where(begin & (ew == plane), 1, 0), axis=0, keepdims=True)
    meta_v[6:7, :] = jnp.where(held > 0, first + 1, 0)
    meta_v[7:8, :] = jnp.zeros((1, LANES), I32)
    meta_copy = pltpu.make_async_copy(meta_v, meta_s, meta_sem)
    meta_copy.start()
    m_v[...] = jnp.zeros_like(m_v)
    meta_copy.wait()

    all_z(lambda zz: over_y(lambda yy: q_y(y, zz * YN + yy).wait_recv()))

    def query_of(b, ch):
        return q_all[(meta_s[b, ch] >> 6) & (2 * G - 1)]

    def passage_of(ch):
        return jnp.maximum((meta_s[0, ch] >> 12) - 1, 0)

    token = iota((token_len, LANES), 0)

    def forward(ch):
        pid = passage_of(ch)
        queries = jnp.concatenate([query_of(b, ch) for b in range(WIDE)], axis=0)
        x = lax.dot_general(
            p_v[pid], queries, (((1,), (1,)), ((), ())), preferred_element_type=F32
        )
        x = jnp.where(token < len_ref[0, pid], x, -1e30)
        highest = jnp.max(x, axis=0, keepdims=True)
        powers = jnp.exp2((x - highest) * SCALE2)
        summed = jnp.sum(powers, axis=0, keepdims=True)
        att[ch] = (powers * (1.0 / summed)).astype(BF16)
        return highest + temper * jnp.log(summed)

    def forward_group(g, carry):
        rows = [forward(g * UNROLL + u) for u in range(UNROLL)]
        m_v[pl.ds(pl.multiple_of(g * UNROLL, UNROLL), UNROLL), :] = jnp.concatenate(rows, axis=0)
        return carry

    lax.fori_loop(0, NCH // UNROLL, forward_group, 0)

    matched = m_v[...]
    block = iota((LANES, LANES), 1) >> 5
    loc_cols = loccol[...]
    scores = jnp.zeros((nslot, 1), F32)
    for b in range(WIDE):
        row = to_row(pick(block == b, matched))
        hit = loc_cols == iota((nslot, LANES), 1) * WIDE + b
        scores += pick(hit, jnp.broadcast_to(row, (nslot, LANES)))
    slots = [slotr[k][:, 0:1] for k in range(CAP)]
    score = [scores[k * G : (k + 1) * G, :] for k in range(CAP)]
    belongs = [[(r >= 0) & (r < 64) for r in slots], [r >= 64 for r in slots]]
    spot = ylane - iota((G, LANES), 0)
    stats = jnp.zeros((1, LANES), F32)
    for h in (0, 1):
        top = jnp.full((G, 1), LOW, F32)
        for k in range(CAP):
            top = jnp.maximum(top, jnp.where(belongs[h][k], score[k], LOW))
        total = jnp.zeros((G, 1), F32)
        for k in range(CAP):
            total += jnp.where(belongs[h][k], jnp.exp(score[k] - top), 0.0)
        for col, shift in ((top, h * G), (total, 64 + h * G)):
            stats += jnp.sum(jnp.where(spot == shift, col, 0.0), axis=0, keepdims=True)
    v_r[me] = stats

    def v_to(to, src):
        return remote(v_r.at[src], v_r.at[src], v_send.at[to], v_recv.at[src], to, rep)

    def over_all(body):
        over_z(lambda zz: [body(zz * YN + lax.rem(y + t, YN)) for t in (2, 1, 3, 0)] and None, far=True)
        over_y(lambda yy: body(z * YN + yy))

    over_all(lambda g: v_to(g, me).start())

    def lift(ch):
        u = lax.dot_general(
            att[ch], p_v[passage_of(ch)], (((0,), (0,)), ((), ())), preferred_element_type=F32
        )
        u_v[pl.ds(ch * WIDE, WIDE)] = u.astype(BF16).reshape(WIDE, query_len, dim)

    def lift_group(g, carry):
        for u in range(UNROLL):
            lift(g * UNROLL + u)
        return carry

    groups = NCH // UNROLL
    lax.fori_loop(0, groups, lift_group, 0)

    teacher = t_r[:, 0, :]
    half = ylane >> 6
    top = [jnp.max(jnp.where(half == h, teacher, LOW), axis=1, keepdims=True) for h in (0, 1)]
    shifted = teacher - jnp.where(half == 0, top[0], top[1])
    powers = jnp.exp(shifted)
    total = [pick(half == h, powers) for h in (0, 1)]
    log_teacher = shifted - jnp.log(jnp.where(half == 0, total[0], total[1]))
    weight = [pick(ylane == h * 64, t_r[:, 1, :]) for h in (0, 1)]

    over_rep(lambda rr: w_rep(rep, rr).wait_recv())
    by_rep = jnp.sum(wr[...], axis=0)
    weight_sum = jnp.sum(jnp.where((lane & 63) == 0, by_rep, 0.0), axis=1, keepdims=True)
    over_all(lambda g: v_to(me, g).wait_recv())
    stats = v_r[:, 0, :]
    top = jnp.max(stats, axis=0, keepdims=True)
    total = jnp.sum(pltpu.roll(stats, 64, 1) * jnp.exp(stats - top), axis=0, keepdims=True)
    log_total = top + jnp.log(total)
    log_totals = [pick(spot == h * G, jnp.broadcast_to(log_total, (G, LANES))) for h in (0, 1)]

    scale_all = 2.0 * G * R
    by_slot = []
    part = jnp.zeros((G, 1), F32)
    for k in range(CAP):
        late = belongs[1][k]
        valid = slots[k] >= 0
        log_t = pick(slotr[k] == ylane, log_teacher)
        log_s = score[k] - jnp.where(late, log_totals[1], log_totals[0])
        w = jnp.where(late, weight[1], weight[0])
        prob_t = jnp.exp(log_t)
        grad = scale_all * w / weight_sum * (jnp.exp(log_s) - prob_t)
        grad = jnp.where(valid, grad, 0.0)
        part += jnp.where(valid, w * (prob_t * (log_t - log_s)), 0.0)
        by_slot.append(grad)
        sgq[:, k, :] = jnp.broadcast_to(jnp.where(late, 0.0, grad), (G, LANES))
        sgq[:, CAP + k, :] = jnp.broadcast_to(jnp.where(late, grad, 0.0), (G, LANES))
    gz_r[z] = jnp.broadcast_to(jnp.sum(part, axis=0, keepdims=True), (1, LANES))

    def g_z(to, src):
        return remote(gz_r.at[src], gz_r.at[src], gz_send.at[to], gz_recv.at[src], to * YN + y, rep)

    def g_y(to, src):
        return remote(gy_r.at[src], gy_r.at[src], gy_send.at[to], gy_recv.at[src], z * YN + to, rep)

    def l_rep(to, src):
        return remote(lr.at[src], lr.at[src], l_send.at[to], l_recv.at[src], me, to)

    over_z(lambda zz: g_z(zz, z).start())

    def query_sum(s):
        scales = sgq[s]
        one = jnp.zeros((query_len, dim), F32)
        two = jnp.zeros((query_len, dim), F32)
        for k in range(CAP):
            e = k * G + s
            at = jnp.maximum(meta_s[WIDE + e // LANES, lax.rem(e, LANES)], 0)
            u = u_v[at].astype(F32)
            one += scales[k : k + 1, :] * u
            two += scales[CAP + k : CAP + k + 1, :] * u
        return one, two

    def o_y(to, zz, src):
        ssem, rsem = oy_send.at[zz * YN + to], oy_recv.at[zz * YN + src]
        dst = oy_r.at[zz * YN + src]
        return remote(oy_s.at[zz * YN + to], dst, ssem, rsem, z * YN + to, rep)

    def o_z(to, src):
        return remote(oz_s.at[to], oz_r.at[src], oz_send.at[to], oz_recv.at[src], to * YN + y, rep)

    def send_sums(zz):
        def one_way(yy):
            one, two = query_sum(zz * YN + yy)
            oy_s[zz * YN + yy, 0] = one.astype(BF16)
            oy_s[zz * YN + yy, 1] = two.astype(BF16)
            o_y(yy, zz, y).start()

        over_y(one_way)

    over_z(send_sums, far=True)
    send_sums(z)

    def keep_sums(zz):
        one, two = query_sum(zz * YN + y)
        own[zz, 0] = one
        own[zz, 1] = two

    all_z(keep_sums)

    sg_row = to_row(jnp.concatenate(by_slot, axis=0))
    loc_rows = jnp.concatenate(
        [meta_v[WIDE + h : WIDE + h + 1, :] for h in range(nslot // LANES)], axis=1
    )
    for b in range(WIDE):
        hit = loc_rows == iota((LANES, nslot), 0) * WIDE + b
        col = pick(hit, jnp.broadcast_to(sg_row, (LANES, nslot)))
        sgl[:, b, :] = jnp.broadcast_to(col, (LANES, LANES))

    acc[...] = jnp.zeros_like(acc)

    def back(ch):
        scales = sgl[ch]
        scaled = jnp.concatenate(
            [
                (query_of(b, ch).astype(F32) * scales[b : b + 1, :]).astype(BF16)
                for b in range(WIDE)
            ],
            axis=0,
        )
        product = jnp.dot(att[ch], scaled, preferred_element_type=F32)
        follows = (meta_s[0, ch] >> 12) == (meta_s[0, ch + 1] >> 12)
        total = product + acc[...] * jnp.where(follows, 1.0, 0.0)
        acc[...] = total
        att[ch] = total.astype(BF16)

    def back_group(i, carry):
        g = groups - 1 - i
        for u in range(UNROLL):
            back(g * UNROLL + UNROLL - 1 - u)
        return carry

    lax.fori_loop(0, groups // 2, back_group, 0)
    over_z(lambda zz: g_z(z, zz).wait_recv())
    gy_r[y] = jnp.sum(gz_r[...], axis=0)
    over_y(lambda yy: g_y(yy, y).start())
    lax.fori_loop(groups // 2, groups, back_group, 0)
    over_y(lambda yy: g_y(y, yy).wait_recv())
    lr[rep] = jnp.sum(gy_r[...], axis=0)
    over_rep(lambda rr: l_rep(rr, rep).start())

    def line_sum(zz):
        total = own[zz]

        for t in range(1, YN):
            yy = lax.rem(y + t, YN)
            o_y(y, zz, yy).wait_recv()
            total += oy_r[zz * YN + yy].astype(F32)
        return total

    def send_line(zz):
        oz_s[zz] = line_sum(zz).astype(BF16)
        o_z(zz, z).start()

    over_z(send_line, far=True)
    own[z] = line_sum(z)

    def place(p, carry):
        mark = meta_s[6, p]
        rows = att[jnp.maximum(mark - 1, 0)].astype(F32) * jnp.where(mark > 0, 1.0, 0.0)
        p_f[pl.ds(p, token_len, stride=stored), :] = rows
        return carry

    lax.fori_loop(0, stored, place, 0)

    def pack(i, carry):
        for u in range(4):
            j = i * 4 + u
            pgrad_ref[j] = p_f[pl.ds(pl.multiple_of(j * stored, stored), stored), :].astype(BF16)
        return carry

    lax.fori_loop(0, token_len // 4, pack, 0)

    over_rep(lambda rr: l_rep(rep, rr).wait_recv())
    loss_ref[...] = jnp.sum(lr[...], axis=0) / weight_sum

    qgrad_ref[...] = own[z]

    def add(zz):
        o_z(z, zz).wait_recv()
        qgrad_ref[...] += oz_r[zz].astype(F32)

    over_z(add)

    def drain_z(zz):
        for copy in (t_z, q_z, g_z, o_z):
            copy(zz, z).wait_send()

    def drain_y(zz, yy):
        t_y(yy, zz * YN + y).wait_send()
        q_y(yy, zz * YN + y).wait_send()
        o_y(yy, zz, y).wait_send()

    over_z(drain_z)
    all_z(lambda zz: over_y(lambda yy: drain_y(zz, yy)))
    over_all(lambda g: v_to(g, me).wait_send())
    over_y(lambda yy: g_y(yy, y).wait_send())
    over_rep(lambda rr: w_rep(rr, rep).wait_send())
    over_rep(lambda rr: l_rep(rr, rep).wait_send())


def on_device(G, R, queries, passages, lengths, cand_ids, owner_map, teacher, weights):
    query_local, _, query_len, dim = queries.shape
    stored, _, token_len, _ = passages.shape
    chunks = (G * CAP + (WIDE - 1) * stored) // WIDE
    NCH = -(-chunks // UNROLL) * UNROLL
    pitch = -(-token_len // 8) * 8
    ZN = G // YN
    vmem = pl.BlockSpec(memory_space=pltpu.VMEM)
    smem = pl.BlockSpec(memory_space=pltpu.SMEM)
    hbm = pl.BlockSpec(memory_space=pl.ANY)
    dma = pltpu.SemaphoreType.DMA
    loss, qgrad, pgrad = pl.pallas_call(
        functools.partial(step_kernel, G, R, NCH),
        out_shape=(
            pltpu.VMEM((1, LANES), F32),
            pltpu.VMEM((query_local, query_len, dim), F32),
            pltpu.VMEM((token_len, stored, dim), BF16),
        ),
        in_specs=[vmem, vmem, vmem, hbm, smem, vmem, smem],
        out_specs=(vmem, vmem, vmem),
        scratch_shapes=[
            pltpu.VMEM((token_len, stored, dim), BF16),
            pltpu.VMEM((stored * pitch, dim), F32),
            pltpu.VMEM((stored, token_len, dim), BF16),
            pltpu.VMEM((query_local * G, query_len, dim), BF16),
            pltpu.VMEM((1, LANES), I32),
            pltpu.VMEM((G, 3, LANES), F32),
            pltpu.VMEM((G, 1, LANES), F32),
            pltpu.VMEM((ZN, 1, LANES), F32),
            pltpu.VMEM((YN, 1, LANES), F32),
            pltpu.VMEM((R, 1, LANES), F32),
            pltpu.VMEM((R, 1, LANES), F32),
            pltpu.VMEM((8, LANES), I32),
            pltpu.SMEM((8, LANES), I32),
            pltpu.VMEM((LANES, LANES), F32),
            pltpu.VMEM((NCH, token_len, LANES), BF16),
            pltpu.VMEM((NCH * WIDE, query_len, dim), BF16),
            pltpu.VMEM((CAP, G, LANES), I32),
            pltpu.VMEM((G * CAP, LANES), I32),
            pltpu.VMEM((G, 2 * CAP, LANES), F32),
            pltpu.VMEM((LANES, WIDE, LANES), F32),
            pltpu.VMEM((G, query_local, query_len, dim), BF16),
            pltpu.VMEM((G, query_local, query_len, dim), BF16),
            pltpu.VMEM((ZN, query_local, query_len, dim), BF16),
            pltpu.VMEM((ZN, query_local, query_len, dim), BF16),
            pltpu.VMEM((ZN, query_local, query_len, dim), F32),
            pltpu.VMEM((token_len, dim), F32),
            dma,
            dma,
        ]
        + [dma((G,))] * 8
        + [dma((ZN,))] * 8
        + [dma((YN,))] * 2
        + [dma((R,))] * 4,
        compiler_params=pltpu.CompilerParams(
            collective_id=0, has_side_effects=True, vmem_limit_bytes=56 * 1024 * 1024
        ),
    )(
        cand_ids,
        owner_map,
        queries.reshape(query_local, query_len, dim),
        jnp.transpose(passages[:, 0], (1, 0, 2)),
        lengths.reshape(1, stored),
        teacher,
        weights.reshape(1, query_local),
    )
    return loss[0, 0], qgrad[:, None], jnp.transpose(pgrad, (1, 0, 2))[:, None]


def solution(mesh):
    G, R = mesh.shape["grp"], mesh.shape["rep"]
    in_specs = (
        P("grp", "rep", None, None),
        P("grp", "rep", None, None),
        P("grp", "rep"),
        P("grp", "rep", None),
        P("rep", None),
        P("grp", "rep", None),
        P("grp", "rep"),
    )
    out_specs = (P(), P("grp", "rep", None, None), P("grp", "rep", None, None))
    return jax.shard_map(
        functools.partial(on_device, G, R),
        mesh=mesh,
        in_specs=in_specs,
        out_specs=out_specs,
        check_vma=False,
    )
```

```python
import functools

import jax
import jax.numpy as jnp
from jax import lax
from jax.experimental import pallas as pl
from jax.experimental.pallas import tpu as pltpu
from jax.sharding import PartitionSpec as P

MESH = pl.DeviceIdType.MESH
F32 = jnp.float32
BF16 = jnp.bfloat16
I32 = jnp.int32

temper = 0.05
SCALE2 = 20.0 * 1.4426950408889634
LANES = 128
CAP = 8
WIDE = 4
UNROLL = 8
PART = 9
LOW = -3e38
YN = 4


def iota(shape, axis):
    return lax.broadcasted_iota(I32, shape, axis)


def to_row(col):
    n = col.shape[0]
    eye = iota((n, n), 0) == iota((n, n), 1)
    return jnp.sum(jnp.where(eye, col, jnp.zeros_like(col)), axis=0, keepdims=True)


def to_col(row):
    n = row.shape[1]
    eye = iota((n, n), 0) == iota((n, n), 1)
    return jnp.sum(jnp.where(eye, row, jnp.zeros_like(row)), axis=1, keepdims=True)


def pick(mask, values):
    return jnp.sum(jnp.where(mask, values, jnp.zeros_like(values)), axis=1, keepdims=True)


def step_kernel(
    G,
    R,
    NCH,
    cand_hbm,
    omap_hbm,
    q_hbm,
    p_hbm,
    len_hbm,
    teach_hbm,
    w_hbm,
    loss_ref,
    qgrad_ref,
    pgrad_ref,
    cand_ref,
    omap_ref,
    q_ref,
    len_ref,
    teach_ref,
    w_ref,
    pt_v,
    p_f,
    p_v,
    q_all,
    c_v,
    t_r,
    v_r,
    gz_r,
    gy_r,
    wr,
    lr,
    meta_v,
    meta_s,
    m_v,
    att,
    u_v,
    slotr,
    loccol,
    sgq,
    sgl,
    oy_s,
    oy_r,
    oz_s,
    oz_r,
    own,
    sums,
    acc,
    in_sem,
    p_sem,
    meta_sem,
    t_sent,
    q_sent,
    v_sent,
    g_sent,
    oy_sent,
    oz_sent,
    w_sent,
    l_sent,
    ty_recv,
    qy_recv,
    v_recv,
    gz_recv,
    gy_recv,
    oz_recv,
    w_recv,
    l_recv,
    tz_recv,
    qz_recv,
    oy_recv,
):
    me = lax.axis_index("grp")
    rep = lax.axis_index("rep")
    ZN = G // YN
    z, y = me // YN, lax.rem(me, YN)
    stored, token_len, dim = p_v.shape
    query_len = q_ref.shape[1]
    nslot = G * CAP

    def remote(src, dst, ssem, rsem, g, r):
        return pltpu.make_async_remote_copy(
            src_ref=src,
            dst_ref=dst,
            send_sem=ssem,
            recv_sem=rsem,
            device_id=(g, r),
            device_id_type=MESH,
        )

    def finish(like, count, sem):
        blocks = like.at[pl.ds(0, count)]
        pltpu.make_async_copy(blocks, blocks, sem).wait()

    def near_z(t):
        odd = lax.rem(t, 2)
        return lax.rem(z + odd * ((t + 1) // 2) + (1 - odd) * (ZN - t // 2), ZN)

    def over_z(body, far=False):
        def one(t, carry):
            body(near_z(ZN - t if far else t))
            return carry

        lax.fori_loop(1, ZN, one, 0)

    def over_y(body):
        for t in range(1, YN):
            body(lax.rem(y + t, YN))

    def over_rep(body):
        for t in range(1, R):
            body(lax.rem(rep + t, R))

    barrier = pltpu.get_barrier_semaphore()

    def greet(g, r):
        pl.semaphore_signal(barrier, inc=1, device_id=(g, r), device_id_type=MESH)

    over_z(lambda zz: greet(zz * YN + y, rep))
    over_y(lambda yy: greet(z * YN + yy, rep))
    over_rep(lambda rr: greet(me, rr))
    inputs = [
        pltpu.make_async_copy(src, dst, in_sem.at[i])
        for i, (src, dst) in enumerate(
            (
                (cand_hbm, cand_ref),
                (omap_hbm, omap_ref),
                (q_hbm, q_ref),
                (teach_hbm, teach_ref),
                (w_hbm, w_ref),
                (len_hbm, len_ref),
            )
        )
    ]
    for copy in inputs:
        copy.start()
    p_copy = pltpu.make_async_copy(p_hbm, pt_v, p_sem)
    p_copy.start()
    for copy in inputs:
        copy.wait()

    c_v[:, 0:64] = cand_ref[0]
    c_v[:, 64:LANES] = cand_ref[1]
    omap = omap_ref[...]
    count = omap.shape[1]
    wanted = to_col(c_v[...])
    pos = pick(wanted == iota((LANES, count), 1), jnp.broadcast_to(omap, (LANES, count)))
    lane = iota((1, LANES), 1)
    t_r[me, 0:1, 0:64] = teach_ref[0]
    t_r[me, 0:1, 64:LANES] = teach_ref[1]
    t_r[me, 1:2, :] = jnp.where(lane < 64, w_ref[0, 0], w_ref[0, 1])
    t_r[me, 2:3, :] = to_row(pos).astype(F32)
    q_all[pl.ds(2 * me, 2)] = q_ref[...]

    pl.semaphore_wait(barrier, ZN - 1 + YN - 1 + R - 1)

    def t_z(to, src):
        g = src * YN + y
        return remote(t_r.at[g], t_r.at[g], t_sent, tz_recv.at[src], to * YN + y, rep)

    def q_z(to, src):
        rows = q_all.at[pl.ds(2 * (src * YN + y), 2)]
        return remote(rows, rows, q_sent, qz_recv.at[src], to * YN + y, rep)

    def t_y(to, g):
        return remote(t_r.at[g], t_r.at[g], t_sent, ty_recv, z * YN + to, rep)

    def q_y(to, g):
        rows = q_all.at[pl.ds(2 * g, 2)]
        return remote(rows, rows, q_sent, qy_recv, z * YN + to, rep)

    over_z(lambda zz: t_z(zz, z).start())
    over_y(lambda yy: t_y(yy, me).start())
    over_z(lambda zz: q_z(zz, z).start())
    over_y(lambda yy: q_y(yy, me).start())

    def pass_t(zz):
        t_z(z, zz).wait_recv()
        over_y(lambda yy: t_y(yy, zz * YN + y).start())

    def pass_q(zz):
        q_z(z, zz).wait_recv()
        over_y(lambda yy: q_y(yy, zz * YN + y).start())

    p_copy.wait()
    pitch = p_f.shape[0] // stored

    def spread(i, carry):
        for u in range(4):
            j = i * 4 + u
            p_f[pl.ds(j, stored, stride=pitch), :] = pt_v[j].astype(F32)
        return carry

    lax.fori_loop(0, token_len // 4, spread, 0)

    def settle(t):
        for u in range(stored // ZN):
            p = t * (stored // ZN) + u
            p_v[p] = p_f[pl.ds(pl.multiple_of(p * pitch, 8), token_len), :].astype(BF16)

    pass_t(near_z(1))

    def pass_on(t, carry):
        pass_t(near_z(t + 1))
        pass_q(near_z(t))
        settle(t)
        return carry

    lax.fori_loop(1, ZN - 1, pass_on, 0)
    pass_q(near_z(ZN - 1))
    settle(0)
    settle(ZN - 1)

    def all_z(body):
        def one(zz, carry):
            body(zz)
            return carry

        lax.fori_loop(0, ZN, one, 0)

    finish(t_r, ZN * (YN - 1), ty_recv)

    wr[rep] = jnp.sum(t_r[:, 1, :], axis=0, keepdims=True)

    def w_rep(to, src):
        return remote(wr.at[src], wr.at[src], w_sent, w_recv, me, to)

    over_rep(lambda rr: w_rep(rr, rep).start())

    spots = t_r[:, 2, :].astype(I32)
    have = (spots >> 6) == me
    lower = (iota((LANES, LANES), 0) < iota((LANES, LANES), 1)).astype(BF16)
    before = jnp.dot(have.astype(F32).astype(BF16), lower, preferred_element_type=F32).astype(I32)
    ylane = iota((G, LANES), 1)
    code = jnp.where(have, (((spots & 63) + 1) << 7) | ylane, 0)
    codes = [pick(have & (before == k), code) for k in range(CAP)]
    for k in range(CAP):
        rk = jnp.where(codes[k] > 0, codes[k] & 127, -1)
        slotr[k] = jnp.broadcast_to(rk, (G, LANES))
    ecode = jnp.concatenate(codes, axis=0)
    ew = ecode >> 7
    er = ecode & 127
    es = jnp.concatenate([iota((G, 1), 0)] * CAP, axis=0)
    ew_row = to_row(ew)
    used_row = ew_row > 0
    same = (ew == ew_row) & used_row
    rank = jnp.sum(
        jnp.where(same & (iota((nslot, nslot), 1) < iota((nslot, nslot), 0)), 1, 0),
        axis=1,
        keepdims=True,
    )
    rank_row = to_row(rank)
    starts = used_row & ((rank_row & (WIDE - 1)) == 0) & (ew_row < ew)
    base = jnp.sum(jnp.where(starts, 1, 0), axis=1, keepdims=True)
    loc = jnp.where(ew > 0, (base + (rank >> 2)) * WIDE + (rank & (WIDE - 1)), -1)
    loccol[...] = jnp.broadcast_to(loc, (nslot, LANES))
    packed = (ew << 12) | (es << 7) | er
    for b in range(WIDE):
        hit = loc == iota((nslot, LANES), 1) * WIDE + b
        meta_v[b : b + 1, :] = jnp.sum(jnp.where(hit, packed, 0), axis=0, keepdims=True)
    loc_row = to_row(loc)
    for h in range(nslot // LANES):
        meta_v[WIDE + h : WIDE + h + 1, :] = loc_row[:, h * LANES : (h + 1) * LANES]
    plane = iota((nslot, LANES), 1) + 1
    begin = (ew > 0) & ((rank & (WIDE - 1)) == 0)
    first = jnp.sum(jnp.where(begin & (ew < plane), 1, 0), axis=0, keepdims=True)
    held = jnp.sum(jnp.where(begin & (ew == plane), 1, 0), axis=0, keepdims=True)
    meta_v[6:7, :] = jnp.where(held > 0, first + 1, 0)
    meta_v[7:8, :] = jnp.zeros((1, LANES), I32)
    meta_copy = pltpu.make_async_copy(meta_v, meta_s, meta_sem)
    meta_copy.start()
    m_v[...] = jnp.zeros_like(m_v)
    meta_copy.wait()

    finish(q_all, 2 * ZN * (YN - 1), qy_recv)

    def query_of(b, ch):
        return q_all[(meta_s[b, ch] >> 6) & (2 * G - 1)]

    def passage_of(ch):
        return jnp.maximum((meta_s[0, ch] >> 12) - 1, 0)

    token = iota((token_len, LANES), 0)

    def forward(ch):
        pid = passage_of(ch)
        queries = jnp.concatenate([query_of(b, ch) for b in range(WIDE)], axis=0)
        x = lax.dot_general(
            p_v[pid], queries, (((1,), (1,)), ((), ())), preferred_element_type=F32
        )
        x = jnp.where(token < len_ref[0, pid], x, -1e30)
        highest = jnp.max(x, axis=0, keepdims=True)
        powers = jnp.exp2((x - highest) * SCALE2)
        summed = jnp.sum(powers, axis=0, keepdims=True)
        att[ch] = (powers * (1.0 / summed)).astype(BF16)
        return highest + temper * jnp.log(summed)

    def forward_group(g, carry):
        rows = [forward(g * UNROLL + u) for u in range(UNROLL)]
        m_v[pl.ds(pl.multiple_of(g * UNROLL, UNROLL), UNROLL), :] = jnp.concatenate(rows, axis=0)
        return carry

    lax.fori_loop(0, NCH // UNROLL, forward_group, 0)

    matched = m_v[...]
    block = iota((LANES, LANES), 1) >> 5
    loc_cols = loccol[...]
    scores = jnp.zeros((nslot, 1), F32)
    for b in range(WIDE):
        row = to_row(pick(block == b, matched))
        hit = loc_cols == iota((nslot, LANES), 1) * WIDE + b
        scores += pick(hit, jnp.broadcast_to(row, (nslot, LANES)))
    slots = [slotr[k][:, 0:1] for k in range(CAP)]
    score = [scores[k * G : (k + 1) * G, :] for k in range(CAP)]
    belongs = [[(r >= 0) & (r < 64) for r in slots], [r >= 64 for r in slots]]
    spot = ylane - iota((G, LANES), 0)
    stats = jnp.zeros((1, LANES), F32)
    for h in (0, 1):
        top = jnp.full((G, 1), LOW, F32)
        for k in range(CAP):
            top = jnp.maximum(top, jnp.where(belongs[h][k], score[k], LOW))
        total = jnp.zeros((G, 1), F32)
        for k in range(CAP):
            total += jnp.where(belongs[h][k], jnp.exp(score[k] - top), 0.0)
        for col, shift in ((top, h * G), (total, 64 + h * G)):
            stats += jnp.sum(jnp.where(spot == shift, col, 0.0), axis=0, keepdims=True)
    v_r[me] = stats

    def v_to(to, src):
        return remote(v_r.at[src], v_r.at[src], v_sent, v_recv, to, rep)

    def over_all(body):
        over_z(lambda zz: [body(zz * YN + lax.rem(y + t, YN)) for t in (2, 1, 3, 0)] and None, far=True)
        over_y(lambda yy: body(z * YN + yy))

    over_all(lambda g: v_to(g, me).start())

    def lift(ch):
        u = lax.dot_general(
            att[ch], p_v[passage_of(ch)], (((0,), (0,)), ((), ())), preferred_element_type=F32
        )
        u_v[pl.ds(ch * WIDE, WIDE)] = u.astype(BF16).reshape(WIDE, query_len, dim)

    def lift_group(g, carry):
        for u in range(UNROLL):
            lift(g * UNROLL + u)
        return carry

    groups = NCH // UNROLL
    lax.fori_loop(0, groups, lift_group, 0)

    teacher = t_r[:, 0, :]
    half = ylane >> 6
    top = [jnp.max(jnp.where(half == h, teacher, LOW), axis=1, keepdims=True) for h in (0, 1)]
    shifted = teacher - jnp.where(half == 0, top[0], top[1])
    powers = jnp.exp(shifted)
    total = [pick(half == h, powers) for h in (0, 1)]
    log_teacher = shifted - jnp.log(jnp.where(half == 0, total[0], total[1]))
    weight = [pick(ylane == h * 64, t_r[:, 1, :]) for h in (0, 1)]

    finish(wr, R - 1, w_recv)
    by_rep = jnp.sum(wr[...], axis=0)
    weight_sum = jnp.sum(jnp.where((lane & 63) == 0, by_rep, 0.0), axis=1, keepdims=True)
    finish(v_r, G - 1, v_recv)
    stats = v_r[:, 0, :]
    top = jnp.max(stats, axis=0, keepdims=True)
    total = jnp.sum(pltpu.roll(stats, 64, 1) * jnp.exp(stats - top), axis=0, keepdims=True)
    log_total = top + jnp.log(total)
    log_totals = [pick(spot == h * G, jnp.broadcast_to(log_total, (G, LANES))) for h in (0, 1)]

    scale_all = 2.0 * G * R
    by_slot = []
    part = jnp.zeros((G, 1), F32)
    for k in range(CAP):
        late = belongs[1][k]
        valid = slots[k] >= 0
        log_t = pick(slotr[k] == ylane, log_teacher)
        log_s = score[k] - jnp.where(late, log_totals[1], log_totals[0])
        w = jnp.where(late, weight[1], weight[0])
        prob_t = jnp.exp(log_t)
        grad = scale_all * w / weight_sum * (jnp.exp(log_s) - prob_t)
        grad = jnp.where(valid, grad, 0.0)
        part += jnp.where(valid, w * (prob_t * (log_t - log_s)), 0.0)
        by_slot.append(grad)
        sgq[:, k, :] = jnp.broadcast_to(jnp.where(late, 0.0, grad), (G, LANES))
        sgq[:, CAP + k, :] = jnp.broadcast_to(jnp.where(late, grad, 0.0), (G, LANES))
    gz_r[z] = jnp.broadcast_to(jnp.sum(part, axis=0, keepdims=True), (1, LANES))

    def g_z(to, src):
        return remote(gz_r.at[src], gz_r.at[src], g_sent, gz_recv, to * YN + y, rep)

    def g_y(to, src):
        return remote(gy_r.at[src], gy_r.at[src], g_sent, gy_recv, z * YN + to, rep)

    def l_rep(to, src):
        return remote(lr.at[src], lr.at[src], l_sent, l_recv, me, to)

    over_z(lambda zz: g_z(zz, z).start())

    def query_sum(s):
        scales = sgq[s]
        one = jnp.zeros((query_len, dim), F32)
        two = jnp.zeros((query_len, dim), F32)
        for k in range(CAP):
            e = k * G + s
            at = jnp.maximum(meta_s[WIDE + e // LANES, lax.rem(e, LANES)], 0)
            u = u_v[at].astype(F32)
            one += scales[k : k + 1, :] * u
            two += scales[CAP + k : CAP + k + 1, :] * u
        return one, two

    def o_y(to, zz, src):
        dst = oy_r.at[zz * YN + src]
        return remote(oy_s.at[zz * YN + to], dst, oy_sent, oy_recv.at[zz], z * YN + to, rep)

    def o_z(to, src):
        return remote(oz_s.at[to], oz_r.at[src], oz_sent, oz_recv, to * YN + y, rep)

    def send_sums(zz):
        def one_way(yy):
            one, two = query_sum(zz * YN + yy)
            oy_s[zz * YN + yy, 0] = one.astype(BF16)
            oy_s[zz * YN + yy, 1] = two.astype(BF16)
            o_y(yy, zz, y).start()

        over_y(one_way)

    over_z(send_sums, far=True)
    send_sums(z)

    def keep_sums(zz):
        one, two = query_sum(zz * YN + y)
        own[zz, 0] = one
        own[zz, 1] = two

    all_z(keep_sums)

    sg_row = to_row(jnp.concatenate(by_slot, axis=0))
    loc_rows = jnp.concatenate(
        [meta_v[WIDE + h : WIDE + h + 1, :] for h in range(nslot // LANES)], axis=1
    )
    for b in range(WIDE):
        hit = loc_rows == iota((LANES, nslot), 0) * WIDE + b
        col = pick(hit, jnp.broadcast_to(sg_row, (LANES, nslot)))
        sgl[:, b, :] = jnp.broadcast_to(col, (LANES, LANES))

    acc[...] = jnp.zeros_like(acc)

    def back(ch, total):
        scales = sgl[ch]
        scaled = jnp.concatenate(
            [
                (query_of(b, ch).astype(F32) * scales[b : b + 1, :]).astype(BF16)
                for b in range(WIDE)
            ],
            axis=0,
        )
        product = jnp.dot(att[ch], scaled, preferred_element_type=F32)
        follows = (meta_s[0, ch] >> 12) == (meta_s[0, ch + 1] >> 12)
        total = product + total * jnp.where(follows, 1.0, 0.0)
        sums[ch] = total.astype(BF16)
        return total

    def back_group(i, carry):
        g = groups - 1 - i
        total = acc[...]
        for u in range(UNROLL):
            total = back(g * UNROLL + UNROLL - 1 - u, total)
        acc[...] = total
        return carry

    lax.fori_loop(0, min(PART, groups), back_group, 0)
    finish(gz_r, ZN - 1, gz_recv)
    gy_r[y] = jnp.sum(gz_r[...], axis=0)
    over_y(lambda yy: g_y(yy, y).start())
    lax.fori_loop(min(PART, groups), groups, back_group, 0)

    def line_sum(zz):
        finish(oy_r, YN - 1, oy_recv.at[zz])
        total = own[zz]
        for t in range(1, YN):
            total += oy_r[zz * YN + lax.rem(y + t, YN)].astype(F32)
        return total

    def send_line(zz):
        oz_s[zz] = line_sum(zz).astype(BF16)
        o_z(zz, z).start()

    over_z(send_line, far=True)
    own[z] = line_sum(z)
    finish(gy_r, YN - 1, gy_recv)
    lr[rep] = jnp.sum(gy_r[...], axis=0)
    over_rep(lambda rr: l_rep(rr, rep).start())

    def place(i, carry):
        for u in range(4):
            p = i * 4 + u
            mark = meta_s[6, p]
            rows = sums[jnp.maximum(mark - 1, 0)].astype(F32) * jnp.where(mark > 0, 1.0, 0.0)
            p_f[pl.ds(p, token_len, stride=stored), :] = rows
        return carry

    lax.fori_loop(0, stored // 4, place, 0)

    def pack(i, carry):
        for u in range(4):
            j = i * 4 + u
            pgrad_ref[j] = p_f[pl.ds(pl.multiple_of(j * stored, stored), stored), :].astype(BF16)
        return carry

    lax.fori_loop(0, token_len // 4, pack, 0)

    finish(t_r, G - 1, t_sent)
    finish(q_all, 2 * (G - 1), q_sent)
    finish(v_r, G - 1, v_sent)
    finish(v_r, ZN + YN - 2, g_sent)
    finish(oy_s, ZN * (YN - 1), oy_sent)
    finish(oz_s, ZN - 1, oz_sent)
    finish(wr, R - 1, w_sent)
    finish(lr, R - 1, l_sent)

    finish(lr, R - 1, l_recv)
    loss_ref[...] = jnp.sum(lr[...], axis=0) / weight_sum

    finish(oz_r, ZN - 1, oz_recv)
    total = own[z]
    for t in range(1, ZN):
        total += oz_r[lax.rem(z + t, ZN)].astype(F32)
    qgrad_ref[...] = total


def on_device(G, R, queries, passages, lengths, cand_ids, owner_map, teacher, weights):
    query_local, _, query_len, dim = queries.shape
    stored, _, token_len, _ = passages.shape
    chunks = (G * CAP + (WIDE - 1) * stored) // WIDE
    NCH = -(-chunks // UNROLL) * UNROLL
    pitch = -(-token_len // 8) * 8
    ZN = G // YN
    vmem = pl.BlockSpec(memory_space=pltpu.VMEM)
    hbm = pl.BlockSpec(memory_space=pl.ANY)
    dma = pltpu.SemaphoreType.DMA
    loss, qgrad, pgrad = pl.pallas_call(
        functools.partial(step_kernel, G, R, NCH),
        out_shape=(
            pltpu.VMEM((1, LANES), F32),
            pltpu.VMEM((query_local, query_len, dim), F32),
            pltpu.VMEM((token_len, stored, dim), BF16),
        ),
        in_specs=[hbm] * 7,
        out_specs=(vmem, vmem, vmem),
        scratch_shapes=[
            pltpu.VMEM(cand_ids.shape, I32),
            pltpu.VMEM(owner_map.shape, I32),
            pltpu.VMEM((query_local, query_len, dim), BF16),
            pltpu.SMEM((1, stored), I32),
            pltpu.VMEM(teacher.shape, F32),
            pltpu.SMEM((1, query_local), F32),
            pltpu.VMEM((token_len, stored, dim), BF16),
            pltpu.VMEM((stored * pitch, dim), F32),
            pltpu.VMEM((stored, token_len, dim), BF16),
            pltpu.VMEM((query_local * G, query_len, dim), BF16),
            pltpu.VMEM((1, LANES), I32),
            pltpu.VMEM((G, 3, LANES), F32),
            pltpu.VMEM((G, 1, LANES), F32),
            pltpu.VMEM((ZN, 1, LANES), F32),
            pltpu.VMEM((YN, 1, LANES), F32),
            pltpu.VMEM((R, 1, LANES), F32),
            pltpu.VMEM((R, 1, LANES), F32),
            pltpu.VMEM((8, LANES), I32),
            pltpu.SMEM((8, LANES), I32),
            pltpu.VMEM((LANES, LANES), F32),
            pltpu.VMEM((NCH, token_len, LANES), BF16),
            pltpu.VMEM((NCH * WIDE, query_len, dim), BF16),
            pltpu.VMEM((CAP, G, LANES), I32),
            pltpu.VMEM((G * CAP, LANES), I32),
            pltpu.VMEM((G, 2 * CAP, LANES), F32),
            pltpu.VMEM((LANES, WIDE, LANES), F32),
            pltpu.VMEM((G, query_local, query_len, dim), BF16),
            pltpu.VMEM((G, query_local, query_len, dim), BF16),
            pltpu.VMEM((ZN, query_local, query_len, dim), BF16),
            pltpu.VMEM((ZN, query_local, query_len, dim), BF16),
            pltpu.VMEM((ZN, query_local, query_len, dim), F32),
            pltpu.VMEM((NCH, token_len, dim), BF16),
            pltpu.VMEM((token_len, dim), F32),
            dma((6,)),
            dma,
            dma,
        ]
        + [dma] * 16
        + [dma((ZN,))] * 3,
        compiler_params=pltpu.CompilerParams(
            collective_id=0, has_side_effects=True, vmem_limit_bytes=56 * 1024 * 1024
        ),
    )(
        cand_ids,
        owner_map,
        queries.reshape(query_local, query_len, dim),
        jnp.transpose(passages[:, 0], (1, 0, 2)),
        lengths.reshape(1, stored),
        teacher,
        weights.reshape(1, query_local),
    )
    return loss[0, 0], qgrad[:, None], jnp.transpose(pgrad, (1, 0, 2))[:, None]


def solution(mesh):
    G, R = mesh.shape["grp"], mesh.shape["rep"]
    in_specs = (
        P("grp", "rep", None, None),
        P("grp", "rep", None, None),
        P("grp", "rep"),
        P("grp", "rep", None),
        P("rep", None),
        P("grp", "rep", None),
        P("grp", "rep"),
    )
    out_specs = (P(), P("grp", "rep", None, None), P("grp", "rep", None, None))
    return jax.shard_map(
        functools.partial(on_device, G, R),
        mesh=mesh,
        in_specs=in_specs,
        out_specs=out_specs,
        check_vma=False,
    )
```

```python
import functools

import jax
import jax.numpy as jnp
from jax import lax
from jax.experimental import pallas as pl
from jax.experimental.pallas import tpu as pltpu
from jax.sharding import PartitionSpec as P

MESH = pl.DeviceIdType.MESH
F32 = jnp.float32
BF16 = jnp.bfloat16
I32 = jnp.int32

temper = 0.05
SCALE2 = 20.0 * 1.4426950408889634
LANES = 128
CAP = 8
WIDE = 4
UNROLL = 16
LOW = -3e38
YN = 4


def iota(shape, axis):
    return lax.broadcasted_iota(I32, shape, axis)


def to_row(col):
    n = col.shape[0]
    eye = iota((n, n), 0) == iota((n, n), 1)
    return jnp.sum(jnp.where(eye, col, jnp.zeros_like(col)), axis=0, keepdims=True)


def to_col(row):
    n = row.shape[1]
    eye = iota((n, n), 0) == iota((n, n), 1)
    return jnp.sum(jnp.where(eye, row, jnp.zeros_like(row)), axis=1, keepdims=True)


def pick(mask, values):
    return jnp.sum(jnp.where(mask, values, jnp.zeros_like(values)), axis=1, keepdims=True)


def step_kernel(
    G,
    R,
    NCH,
    cand_hbm,
    omap_hbm,
    q_hbm,
    p_hbm,
    len_hbm,
    teach_hbm,
    w_hbm,
    loss_ref,
    qgrad_ref,
    pgrad_ref,
    cand_ref,
    omap_ref,
    q_ref,
    len_ref,
    teach_ref,
    w_ref,
    pt_v,
    p_f,
    p_v,
    q_all,
    c_v,
    t_r,
    v_r,
    g_r,
    wr,
    lr,
    meta_v,
    meta_s,
    m_v,
    att,
    u_v,
    slotr,
    loccol,
    sgq,
    sgl,
    oy_s,
    oy_r,
    oz_s,
    oz_r,
    own,
    sums,
    acc,
    in_sem,
    p_sem,
    meta_sem,
    t_sent,
    q_sent,
    v_sent,
    g_sent,
    oy_sent,
    oz_sent,
    w_sent,
    l_sent,
    ty_recv,
    qy_recv,
    v_recv,
    g_recv,
    oz_recv,
    w_recv,
    l_recv,
    tz_recv,
    qz_recv,
    oy_recv,
):
    me = lax.axis_index("grp")
    rep = lax.axis_index("rep")
    ZN = G // YN
    z, y = me // YN, lax.rem(me, YN)
    stored, token_len, dim = p_v.shape
    query_len = q_ref.shape[1]
    nslot = G * CAP

    def remote(src, dst, ssem, rsem, g, r):
        return pltpu.make_async_remote_copy(
            src_ref=src,
            dst_ref=dst,
            send_sem=ssem,
            recv_sem=rsem,
            device_id=(g, r),
            device_id_type=MESH,
        )

    def finish(like, count, sem):
        blocks = like.at[pl.ds(0, count)]
        pltpu.make_async_copy(blocks, blocks, sem).wait()

    def near_z(t):
        odd = lax.rem(t, 2)
        return lax.rem(z + odd * ((t + 1) // 2) + (1 - odd) * (ZN - t // 2), ZN)

    def over_z(body, far=False):
        def one(t, carry):
            body(near_z(ZN - t if far else t))
            return carry

        lax.fori_loop(1, ZN, one, 0)

    def over_y(body):
        for t in range(1, YN):
            body(lax.rem(y + t, YN))

    def over_rep(body):
        for t in range(1, R):
            body(lax.rem(rep + t, R))

    barrier = pltpu.get_barrier_semaphore()

    def greet(g, r):
        pl.semaphore_signal(barrier, inc=1, device_id=(g, r), device_id_type=MESH)

    over_z(lambda zz: greet(zz * YN + y, rep))
    over_y(lambda yy: greet(z * YN + yy, rep))
    over_rep(lambda rr: greet(me, rr))
    inputs = [
        pltpu.make_async_copy(src, dst, in_sem.at[i])
        for i, (src, dst) in enumerate(
            (
                (cand_hbm, cand_ref),
                (omap_hbm, omap_ref),
                (q_hbm, q_ref),
                (teach_hbm, teach_ref),
                (w_hbm, w_ref),
                (len_hbm, len_ref),
            )
        )
    ]
    for copy in inputs:
        copy.start()
    p_copy = pltpu.make_async_copy(p_hbm, pt_v, p_sem)
    p_copy.start()
    for copy in inputs:
        copy.wait()

    c_v[:, 0:64] = cand_ref[0]
    c_v[:, 64:LANES] = cand_ref[1]
    omap = omap_ref[...]
    count = omap.shape[1]
    wanted = to_col(c_v[...])
    pos = pick(wanted == iota((LANES, count), 1), jnp.broadcast_to(omap, (LANES, count)))
    lane = iota((1, LANES), 1)
    t_r[me, 0:1, 0:64] = teach_ref[0]
    t_r[me, 0:1, 64:LANES] = teach_ref[1]
    t_r[me, 1:2, :] = jnp.where(lane < 64, w_ref[0, 0], w_ref[0, 1])
    t_r[me, 2:3, :] = to_row(pos).astype(F32)
    q_all[pl.ds(2 * me, 2)] = q_ref[...]

    pl.semaphore_wait(barrier, ZN - 1 + YN - 1 + R - 1)

    def t_z(to, src):
        g = src * YN + y
        return remote(t_r.at[g], t_r.at[g], t_sent, tz_recv.at[src], to * YN + y, rep)

    def q_z(to, src):
        rows = q_all.at[pl.ds(2 * (src * YN + y), 2)]
        return remote(rows, rows, q_sent, qz_recv.at[src], to * YN + y, rep)

    def t_y(to, g):
        return remote(t_r.at[g], t_r.at[g], t_sent, ty_recv, z * YN + to, rep)

    def q_y(to, g):
        rows = q_all.at[pl.ds(2 * g, 2)]
        return remote(rows, rows, q_sent, qy_recv, z * YN + to, rep)

    over_z(lambda zz: t_z(zz, z).start())
    over_y(lambda yy: t_y(yy, me).start())
    over_z(lambda zz: q_z(zz, z).start())
    over_y(lambda yy: q_y(yy, me).start())

    def pass_t(zz):
        t_z(z, zz).wait_recv()
        over_y(lambda yy: t_y(yy, zz * YN + y).start())

    def pass_q(zz):
        q_z(z, zz).wait_recv()
        over_y(lambda yy: q_y(yy, zz * YN + y).start())

    p_copy.wait()
    pitch = p_f.shape[0] // stored

    def spread(i, carry):
        for u in range(4):
            j = i * 4 + u
            p_f[pl.ds(j, stored, stride=pitch), :] = pt_v[j].astype(F32)
        return carry

    lax.fori_loop(0, token_len // 4, spread, 0)

    def settle(t):
        for u in range(stored // ZN):
            p = t * (stored // ZN) + u
            p_v[p] = p_f[pl.ds(pl.multiple_of(p * pitch, 8), token_len), :].astype(BF16)

    pass_t(near_z(1))

    def pass_on(t, carry):
        pass_t(near_z(t + 1))
        pass_q(near_z(t))
        settle(t)
        return carry

    lax.fori_loop(1, ZN - 1, pass_on, 0)
    pass_q(near_z(ZN - 1))
    settle(0)
    settle(ZN - 1)

    def all_z(body):
        def one(zz, carry):
            body(zz)
            return carry

        lax.fori_loop(0, ZN, one, 0)

    finish(t_r, ZN * (YN - 1), ty_recv)

    wr[rep] = jnp.sum(t_r[:, 1, :], axis=0, keepdims=True)

    def w_rep(to, src):
        return remote(wr.at[src], wr.at[src], w_sent, w_recv, me, to)

    over_rep(lambda rr: w_rep(rr, rep).start())

    spots = t_r[:, 2, :].astype(I32)
    have = (spots >> 6) == me
    lower = (iota((LANES, LANES), 0) < iota((LANES, LANES), 1)).astype(BF16)
    before = jnp.dot(have.astype(F32).astype(BF16), lower, preferred_element_type=F32).astype(I32)
    ylane = iota((G, LANES), 1)
    code = jnp.where(have, (((spots & 63) + 1) << 7) | ylane, 0)
    codes = [pick(have & (before == k), code) for k in range(CAP)]
    for k in range(CAP):
        rk = jnp.where(codes[k] > 0, codes[k] & 127, -1)
        slotr[k] = jnp.broadcast_to(rk, (G, LANES))
    ecode = jnp.concatenate(codes, axis=0)
    ew = ecode >> 7
    er = ecode & 127
    es = jnp.concatenate([iota((G, 1), 0)] * CAP, axis=0)
    ew_row = to_row(ew)
    used_row = ew_row > 0
    same = (ew == ew_row) & used_row
    rank = jnp.sum(
        jnp.where(same & (iota((nslot, nslot), 1) < iota((nslot, nslot), 0)), 1, 0),
        axis=1,
        keepdims=True,
    )
    rank_row = to_row(rank)
    starts = used_row & ((rank_row & (WIDE - 1)) == 0) & (ew_row < ew)
    base = jnp.sum(jnp.where(starts, 1, 0), axis=1, keepdims=True)
    loc = jnp.where(ew > 0, (base + (rank >> 2)) * WIDE + (rank & (WIDE - 1)), -1)
    loccol[...] = jnp.broadcast_to(loc, (nslot, LANES))
    packed = (ew << 12) | (es << 7) | er
    for b in range(WIDE):
        hit = loc == iota((nslot, LANES), 1) * WIDE + b
        meta_v[b : b + 1, :] = jnp.sum(jnp.where(hit, packed, 0), axis=0, keepdims=True)
    loc_row = to_row(loc)
    for h in range(nslot // LANES):
        meta_v[WIDE + h : WIDE + h + 1, :] = loc_row[:, h * LANES : (h + 1) * LANES]
    plane = iota((nslot, LANES), 1) + 1
    begin = (ew > 0) & ((rank & (WIDE - 1)) == 0)
    first = jnp.sum(jnp.where(begin & (ew < plane), 1, 0), axis=0, keepdims=True)
    held = jnp.sum(jnp.where(begin & (ew == plane), 1, 0), axis=0, keepdims=True)
    meta_v[6:7, :] = jnp.where(held > 0, first + 1, 0)
    meta_v[7:8, :] = jnp.zeros((1, LANES), I32)
    meta_copy = pltpu.make_async_copy(meta_v, meta_s, meta_sem)
    meta_copy.start()
    m_v[...] = jnp.zeros_like(m_v)
    meta_copy.wait()

    finish(q_all, 2 * ZN * (YN - 1), qy_recv)

    def query_of(b, ch):
        return q_all[(meta_s[b, ch] >> 6) & (2 * G - 1)]

    def passage_of(ch):
        return jnp.maximum((meta_s[0, ch] >> 12) - 1, 0)

    token = iota((token_len, LANES), 0)

    def forward(ch):
        pid = passage_of(ch)
        queries = jnp.concatenate([query_of(b, ch) for b in range(WIDE)], axis=0)
        x = lax.dot_general(
            p_v[pid], queries, (((1,), (1,)), ((), ())), preferred_element_type=F32
        )
        x = jnp.where(token < len_ref[0, pid], x, -1e30)
        highest = jnp.max(x, axis=0, keepdims=True)
        powers = jnp.exp2((x - highest) * SCALE2)
        summed = jnp.sum(powers, axis=0, keepdims=True)
        att[ch] = (powers * (1.0 / summed)).astype(BF16)
        return highest + temper * jnp.log(summed)

    def forward_group(g, carry):
        rows = [forward(g * UNROLL + u) for u in range(UNROLL)]
        m_v[pl.ds(pl.multiple_of(g * UNROLL, UNROLL), UNROLL), :] = jnp.concatenate(rows, axis=0)
        return carry

    lax.fori_loop(0, NCH // UNROLL, forward_group, 0)

    matched = m_v[...]
    block = iota((LANES, LANES), 1) >> 5
    loc_cols = loccol[...]
    scores = jnp.zeros((nslot, 1), F32)
    for b in range(WIDE):
        row = to_row(pick(block == b, matched))
        hit = loc_cols == iota((nslot, LANES), 1) * WIDE + b
        scores += pick(hit, jnp.broadcast_to(row, (nslot, LANES)))
    slots = [slotr[k][:, 0:1] for k in range(CAP)]
    score = [scores[k * G : (k + 1) * G, :] for k in range(CAP)]
    belongs = [[(r >= 0) & (r < 64) for r in slots], [r >= 64 for r in slots]]
    spot = ylane - iota((G, LANES), 0)
    stats = jnp.zeros((1, LANES), F32)
    for h in (0, 1):
        top = jnp.full((G, 1), LOW, F32)
        for k in range(CAP):
            top = jnp.maximum(top, jnp.where(belongs[h][k], score[k], LOW))
        total = jnp.zeros((G, 1), F32)
        for k in range(CAP):
            total += jnp.where(belongs[h][k], jnp.exp(score[k] - top), 0.0)
        for col, shift in ((top, h * G), (total, 64 + h * G)):
            stats += jnp.sum(jnp.where(spot == shift, col, 0.0), axis=0, keepdims=True)
    v_r[me] = stats

    def v_to(to, src):
        return remote(v_r.at[src], v_r.at[src], v_sent, v_recv, to, rep)

    def over_all(body):
        over_z(lambda zz: [body(zz * YN + lax.rem(y + t, YN)) for t in (2, 1, 3, 0)] and None, far=True)
        over_y(lambda yy: body(z * YN + yy))

    over_all(lambda g: v_to(g, me).start())

    def lift(ch):
        u = lax.dot_general(
            att[ch], p_v[passage_of(ch)], (((0,), (0,)), ((), ())), preferred_element_type=F32
        )
        u_v[pl.ds(ch * WIDE, WIDE)] = u.astype(BF16).reshape(WIDE, query_len, dim)

    def lift_group(g, carry):
        for u in range(UNROLL):
            lift(g * UNROLL + u)
        return carry

    groups = NCH // UNROLL
    lax.fori_loop(0, groups, lift_group, 0)

    teacher = t_r[:, 0, :]
    half = ylane >> 6
    top = [jnp.max(jnp.where(half == h, teacher, LOW), axis=1, keepdims=True) for h in (0, 1)]
    shifted = teacher - jnp.where(half == 0, top[0], top[1])
    powers = jnp.exp(shifted)
    total = [pick(half == h, powers) for h in (0, 1)]
    log_teacher = shifted - jnp.log(jnp.where(half == 0, total[0], total[1]))
    weight = [pick(ylane == h * 64, t_r[:, 1, :]) for h in (0, 1)]

    finish(wr, R - 1, w_recv)
    by_rep = jnp.sum(wr[...], axis=0)
    weight_sum = jnp.sum(jnp.where((lane & 63) == 0, by_rep, 0.0), axis=1, keepdims=True)
    finish(v_r, G - 1, v_recv)
    stats = v_r[:, 0, :]
    top = jnp.max(stats, axis=0, keepdims=True)
    total = jnp.sum(pltpu.roll(stats, 64, 1) * jnp.exp(stats - top), axis=0, keepdims=True)
    log_total = top + jnp.log(total)
    log_totals = [pick(spot == h * G, jnp.broadcast_to(log_total, (G, LANES))) for h in (0, 1)]

    scale_all = 2.0 * G * R
    by_slot = []
    part = jnp.zeros((G, 1), F32)
    for k in range(CAP):
        late = belongs[1][k]
        valid = slots[k] >= 0
        log_t = pick(slotr[k] == ylane, log_teacher)
        log_s = score[k] - jnp.where(late, log_totals[1], log_totals[0])
        w = jnp.where(late, weight[1], weight[0])
        prob_t = jnp.exp(log_t)
        grad = scale_all * w / weight_sum * (jnp.exp(log_s) - prob_t)
        grad = jnp.where(valid, grad, 0.0)
        part += jnp.where(valid, w * (prob_t * (log_t - log_s)), 0.0)
        by_slot.append(grad)
        sgq[:, k, :] = jnp.broadcast_to(jnp.where(late, 0.0, grad), (G, LANES))
        sgq[:, CAP + k, :] = jnp.broadcast_to(jnp.where(late, grad, 0.0), (G, LANES))
    g_r[me] = jnp.broadcast_to(jnp.sum(part, axis=0, keepdims=True), (1, LANES))

    def g_to(to):
        return remote(g_r.at[me], g_r.at[me], g_sent, g_recv, to, rep)

    def l_rep(to, src):
        return remote(lr.at[src], lr.at[src], l_sent, l_recv, me, to)

    def query_sum(s):
        scales = sgq[s]
        one = jnp.zeros((query_len, dim), F32)
        two = jnp.zeros((query_len, dim), F32)
        for k in range(CAP):
            e = k * G + s
            at = jnp.maximum(meta_s[WIDE + e // LANES, lax.rem(e, LANES)], 0)
            u = u_v[at].astype(F32)
            one += scales[k : k + 1, :] * u
            two += scales[CAP + k : CAP + k + 1, :] * u
        return one, two

    def o_y(to, zz, src):
        dst = oy_r.at[zz * YN + src]
        return remote(oy_s.at[zz * YN + to], dst, oy_sent, oy_recv.at[zz], z * YN + to, rep)

    def o_z(to, src):
        return remote(oz_s.at[to], oz_r.at[src], oz_sent, oz_recv, to * YN + y, rep)

    def send_sums(zz):
        def one_way(yy):
            one, two = query_sum(zz * YN + yy)
            oy_s[zz * YN + yy, 0] = one.astype(BF16)
            oy_s[zz * YN + yy, 1] = two.astype(BF16)
            o_y(yy, zz, y).start()

        over_y(one_way)

    def send_sums_and_part(zz):
        send_sums(zz)
        for yy in range(YN):
            g_to(zz * YN + yy).start()

    over_z(send_sums_and_part, far=True)
    send_sums(z)
    over_y(lambda yy: g_to(z * YN + yy).start())

    def keep_sums(zz):
        one, two = query_sum(zz * YN + y)
        own[zz, 0] = one
        own[zz, 1] = two

    all_z(keep_sums)

    sg_row = to_row(jnp.concatenate(by_slot, axis=0))
    loc_rows = jnp.concatenate(
        [meta_v[WIDE + h : WIDE + h + 1, :] for h in range(nslot // LANES)], axis=1
    )
    for b in range(WIDE):
        hit = loc_rows == iota((LANES, nslot), 0) * WIDE + b
        col = pick(hit, jnp.broadcast_to(sg_row, (LANES, nslot)))
        sgl[:, b, :] = jnp.broadcast_to(col, (LANES, LANES))

    acc[...] = jnp.zeros_like(acc)

    def back(ch, total):
        scales = sgl[ch]
        scaled = jnp.concatenate(
            [
                (query_of(b, ch).astype(F32) * scales[b : b + 1, :]).astype(BF16)
                for b in range(WIDE)
            ],
            axis=0,
        )
        product = jnp.dot(att[ch], scaled, preferred_element_type=F32)
        follows = (meta_s[0, ch] >> 12) == (meta_s[0, ch + 1] >> 12)
        total = product + total * jnp.where(follows, 1.0, 0.0)
        sums[ch] = total.astype(BF16)
        return total

    def back_group(i, carry):
        g = groups - 1 - i
        total = acc[...]
        for u in range(UNROLL):
            total = back(g * UNROLL + UNROLL - 1 - u, total)
        acc[...] = total
        return carry

    def line_sum(zz):
        finish(oy_r, YN - 1, oy_recv.at[zz])
        total = own[zz]
        for t in range(1, YN):
            total += oy_r[zz * YN + lax.rem(y + t, YN)].astype(F32)
        return total

    def send_line(zz):
        oz_s[zz] = line_sum(zz).astype(BF16)
        o_z(zz, z).start()

    share = groups // (ZN - 1)

    def send_between(t, carry):
        lax.fori_loop((t - 1) * share, t * share, back_group, 0)
        send_line(near_z(ZN - t))
        return carry

    lax.fori_loop(1, ZN, send_between, 0)
    lax.fori_loop(share * (ZN - 1), groups, back_group, 0)
    own[z] = line_sum(z)
    finish(g_r, G - 1, g_recv)
    lr[rep] = jnp.sum(g_r[...], axis=0)
    over_rep(lambda rr: l_rep(rr, rep).start())

    def place(i, carry):
        for u in range(4):
            p = i * 4 + u
            mark = meta_s[6, p]
            rows = sums[jnp.maximum(mark - 1, 0)].astype(F32) * jnp.where(mark > 0, 1.0, 0.0)
            p_f[pl.ds(p, token_len, stride=stored), :] = rows
        return carry

    lax.fori_loop(0, stored // 4, place, 0)

    def pack(i, carry):
        for u in range(4):
            j = i * 4 + u
            pgrad_ref[j] = p_f[pl.ds(pl.multiple_of(j * stored, stored), stored), :].astype(BF16)
        return carry

    lax.fori_loop(0, token_len // 4, pack, 0)

    finish(t_r, G - 1, t_sent)
    finish(q_all, 2 * (G - 1), q_sent)
    finish(v_r, G - 1, v_sent)
    finish(g_r, G - 1, g_sent)
    finish(oy_s, ZN * (YN - 1), oy_sent)
    finish(oz_s, ZN - 1, oz_sent)
    finish(wr, R - 1, w_sent)
    finish(lr, R - 1, l_sent)

    finish(lr, R - 1, l_recv)
    loss_ref[...] = jnp.sum(lr[...], axis=0) / weight_sum

    finish(oz_r, ZN - 1, oz_recv)
    total = own[z]
    for t in range(1, ZN):
        total += oz_r[lax.rem(z + t, ZN)].astype(F32)
    qgrad_ref[...] = total


def on_device(G, R, queries, passages, lengths, cand_ids, owner_map, teacher, weights):
    query_local, _, query_len, dim = queries.shape
    stored, _, token_len, _ = passages.shape
    chunks = (G * CAP + (WIDE - 1) * stored) // WIDE
    NCH = -(-chunks // UNROLL) * UNROLL
    pitch = -(-token_len // 8) * 8
    ZN = G // YN
    vmem = pl.BlockSpec(memory_space=pltpu.VMEM)
    hbm = pl.BlockSpec(memory_space=pl.ANY)
    dma = pltpu.SemaphoreType.DMA
    loss, qgrad, pgrad = pl.pallas_call(
        functools.partial(step_kernel, G, R, NCH),
        out_shape=(
            pltpu.VMEM((1, LANES), F32),
            pltpu.VMEM((query_local, query_len, dim), F32),
            pltpu.VMEM((token_len, stored, dim), BF16),
        ),
        in_specs=[hbm] * 7,
        out_specs=(vmem, vmem, vmem),
        scratch_shapes=[
            pltpu.VMEM(cand_ids.shape, I32),
            pltpu.VMEM(owner_map.shape, I32),
            pltpu.VMEM((query_local, query_len, dim), BF16),
            pltpu.SMEM((1, stored), I32),
            pltpu.VMEM(teacher.shape, F32),
            pltpu.SMEM((1, query_local), F32),
            pltpu.VMEM((token_len, stored, dim), BF16),
            pltpu.VMEM((stored * pitch, dim), F32),
            pltpu.VMEM((stored, token_len, dim), BF16),
            pltpu.VMEM((query_local * G, query_len, dim), BF16),
            pltpu.VMEM((1, LANES), I32),
            pltpu.VMEM((G, 3, LANES), F32),
            pltpu.VMEM((G, 1, LANES), F32),
            pltpu.VMEM((G, 1, LANES), F32),
            pltpu.VMEM((R, 1, LANES), F32),
            pltpu.VMEM((R, 1, LANES), F32),
            pltpu.VMEM((8, LANES), I32),
            pltpu.SMEM((8, LANES), I32),
            pltpu.VMEM((LANES, LANES), F32),
            pltpu.VMEM((NCH, token_len, LANES), BF16),
            pltpu.VMEM((NCH * WIDE, query_len, dim), BF16),
            pltpu.VMEM((CAP, G, LANES), I32),
            pltpu.VMEM((G * CAP, LANES), I32),
            pltpu.VMEM((G, 2 * CAP, LANES), F32),
            pltpu.VMEM((LANES, WIDE, LANES), F32),
            pltpu.VMEM((G, query_local, query_len, dim), BF16),
            pltpu.VMEM((G, query_local, query_len, dim), BF16),
            pltpu.VMEM((ZN, query_local, query_len, dim), BF16),
            pltpu.VMEM((ZN, query_local, query_len, dim), BF16),
            pltpu.VMEM((ZN, query_local, query_len, dim), F32),
            pltpu.VMEM((NCH, token_len, dim), BF16),
            pltpu.VMEM((token_len, dim), F32),
            dma((6,)),
            dma,
            dma,
        ]
        + [dma] * 15
        + [dma((ZN,))] * 3,
        compiler_params=pltpu.CompilerParams(
            collective_id=0, has_side_effects=True, vmem_limit_bytes=56 * 1024 * 1024
        ),
    )(
        cand_ids,
        owner_map,
        queries.reshape(query_local, query_len, dim),
        jnp.transpose(passages[:, 0], (1, 0, 2)),
        lengths.reshape(1, stored),
        teacher,
        weights.reshape(1, query_local),
    )
    return loss[0, 0], qgrad[:, None], jnp.transpose(pgrad, (1, 0, 2))[:, None]


def solution(mesh):
    G, R = mesh.shape["grp"], mesh.shape["rep"]
    in_specs = (
        P("grp", "rep", None, None),
        P("grp", "rep", None, None),
        P("grp", "rep"),
        P("grp", "rep", None),
        P("rep", None),
        P("grp", "rep", None),
        P("grp", "rep"),
    )
    out_specs = (P(), P("grp", "rep", None, None), P("grp", "rep", None, None))
    return jax.shard_map(
        functools.partial(on_device, G, R),
        mesh=mesh,
        in_specs=in_specs,
        out_specs=out_specs,
        check_vma=False,
    )
```

```python
import functools

import jax
import jax.numpy as jnp
from jax import lax
from jax.experimental import pallas as pl
from jax.experimental.pallas import tpu as pltpu
from jax.sharding import PartitionSpec as P

MESH = pl.DeviceIdType.MESH
F32 = jnp.float32
BF16 = jnp.bfloat16
I32 = jnp.int32

temper = 0.05
SCALE2 = 20.0 * 1.4426950408889634
LANES = 128
CAP = 8
WIDE = 4
UNROLL = 16
FWD, LIFT = 56, 28
LOW = -3e38
YN = 4


def iota(shape, axis):
    return lax.broadcasted_iota(I32, shape, axis)


def to_row(col):
    n = col.shape[0]
    eye = iota((n, n), 0) == iota((n, n), 1)
    return jnp.sum(jnp.where(eye, col, jnp.zeros_like(col)), axis=0, keepdims=True)


def to_col(row):
    n = row.shape[1]
    eye = iota((n, n), 0) == iota((n, n), 1)
    return jnp.sum(jnp.where(eye, row, jnp.zeros_like(row)), axis=1, keepdims=True)


def pick(mask, values):
    return jnp.sum(jnp.where(mask, values, jnp.zeros_like(values)), axis=1, keepdims=True)


def step_kernel(
    G,
    R,
    NCH,
    cand_hbm,
    omap_hbm,
    q_hbm,
    p_hbm,
    len_hbm,
    teach_hbm,
    w_hbm,
    loss_ref,
    qgrad_ref,
    pgrad_ref,
    cand_ref,
    omap_ref,
    q_ref,
    len_ref,
    teach_ref,
    w_ref,
    pt_v,
    p_f,
    p_v,
    q_all,
    c_v,
    t_r,
    v_r,
    g_r,
    wr,
    lr,
    meta_v,
    meta_s,
    m_v,
    att,
    u_v,
    slotr,
    loccol,
    sgq,
    sgl,
    oy_s,
    oy_r,
    oz_s,
    oz_r,
    own,
    sums,
    acc,
    in_sem,
    p_sem,
    meta_sem,
    t_sent,
    q_sent,
    v_sent,
    g_sent,
    oy_sent,
    oz_sent,
    w_sent,
    l_sent,
    ty_recv,
    qy_recv,
    v_recv,
    g_recv,
    oz_recv,
    w_recv,
    l_recv,
    tz_recv,
    qz_recv,
    oy_recv,
):
    me = lax.axis_index("grp")
    rep = lax.axis_index("rep")
    ZN = G // YN
    z, y = me // YN, lax.rem(me, YN)
    stored, token_len, dim = p_v.shape
    query_len = q_ref.shape[1]
    nslot = G * CAP

    def remote(src, dst, ssem, rsem, g, r):
        return pltpu.make_async_remote_copy(
            src_ref=src,
            dst_ref=dst,
            send_sem=ssem,
            recv_sem=rsem,
            device_id=(g, r),
            device_id_type=MESH,
        )

    def finish(like, count, sem):
        blocks = like.at[pl.ds(0, count)]
        pltpu.make_async_copy(blocks, blocks, sem).wait()

    def near_z(t):
        odd = lax.rem(t, 2)
        return lax.rem(z + odd * ((t + 1) // 2) + (1 - odd) * (ZN - t // 2), ZN)

    def over_z(body, far=False):
        for t in range(1, ZN):
            t = ZN - t if far else t
            body(lax.rem(z + ((t + 1) // 2 if t % 2 else ZN - t // 2), ZN))

    def over_y(body):
        for t in range(1, YN):
            body(lax.rem(y + t, YN))

    def over_rep(body):
        for t in range(1, R):
            body(lax.rem(rep + t, R))

    barrier = pltpu.get_barrier_semaphore()

    def greet(g, r):
        pl.semaphore_signal(barrier, inc=1, device_id=(g, r), device_id_type=MESH)

    over_z(lambda zz: greet(zz * YN + y, rep))
    over_y(lambda yy: greet(z * YN + yy, rep))
    over_rep(lambda rr: greet(me, rr))
    inputs = [
        pltpu.make_async_copy(src, dst, in_sem.at[i])
        for i, (src, dst) in enumerate(
            (
                (cand_hbm, cand_ref),
                (omap_hbm, omap_ref),
                (q_hbm, q_ref),
                (teach_hbm, teach_ref),
                (w_hbm, w_ref),
                (len_hbm, len_ref),
            )
        )
    ]
    for copy in inputs:
        copy.start()
    p_copy = pltpu.make_async_copy(p_hbm, pt_v, p_sem)
    p_copy.start()
    for copy in inputs:
        copy.wait()

    c_v[:, 0:64] = cand_ref[0]
    c_v[:, 64:LANES] = cand_ref[1]
    omap = omap_ref[...]
    count = omap.shape[1]
    wanted = to_col(c_v[...])
    pos = pick(wanted == iota((LANES, count), 1), jnp.broadcast_to(omap, (LANES, count)))
    lane = iota((1, LANES), 1)
    t_r[me, 0:1, 0:64] = teach_ref[0]
    t_r[me, 0:1, 64:LANES] = teach_ref[1]
    t_r[me, 1:2, :] = jnp.where(lane < 64, w_ref[0, 0], w_ref[0, 1])
    t_r[me, 2:3, :] = to_row(pos).astype(F32)
    q_all[pl.ds(2 * me, 2)] = q_ref[...]

    pl.semaphore_wait(barrier, ZN - 1 + YN - 1 + R - 1)

    def t_z(to, src):
        g = src * YN + y
        return remote(t_r.at[g], t_r.at[g], t_sent, tz_recv.at[src], to * YN + y, rep)

    def q_z(to, src):
        rows = q_all.at[pl.ds(2 * (src * YN + y), 2)]
        return remote(rows, rows, q_sent, qz_recv.at[src], to * YN + y, rep)

    def t_y(to, g):
        return remote(t_r.at[g], t_r.at[g], t_sent, ty_recv, z * YN + to, rep)

    def q_y(to, g):
        rows = q_all.at[pl.ds(2 * g, 2)]
        return remote(rows, rows, q_sent, qy_recv, z * YN + to, rep)

    over_z(lambda zz: t_z(zz, z).start())
    over_y(lambda yy: t_y(yy, me).start())
    over_z(lambda zz: q_z(zz, z).start())
    over_y(lambda yy: q_y(yy, me).start())

    def pass_t(zz):
        t_z(z, zz).wait_recv()
        over_y(lambda yy: t_y(yy, zz * YN + y).start())

    def pass_q(zz):
        q_z(z, zz).wait_recv()
        over_y(lambda yy: q_y(yy, zz * YN + y).start())

    p_copy.wait()
    pitch = p_f.shape[0] // stored

    def spread(i, carry):
        for u in range(12):
            j = i * 12 + u
            p_f[pl.ds(j, stored, stride=pitch), :] = pt_v[j].astype(F32)
        return carry

    lax.fori_loop(0, token_len // 12, spread, 0)

    def settle(t):
        for u in range(stored // ZN):
            p = t * (stored // ZN) + u
            p_v[p] = p_f[pl.ds(pl.multiple_of(p * pitch, 8), token_len), :].astype(BF16)

    pass_t(near_z(1))

    def pass_on(t, carry):
        pass_t(near_z(t + 1))
        pass_q(near_z(t))
        settle(t)
        return carry

    lax.fori_loop(1, ZN - 1, pass_on, 0)
    pass_q(near_z(ZN - 1))
    settle(0)
    settle(ZN - 1)

    def all_z(body):
        def one(zz, carry):
            body(zz)
            return carry

        lax.fori_loop(0, ZN, one, 0)

    finish(t_r, ZN * (YN - 1), ty_recv)

    wr[rep] = jnp.sum(t_r[:, 1, :], axis=0, keepdims=True)

    def w_rep(to, src):
        return remote(wr.at[src], wr.at[src], w_sent, w_recv, me, to)

    over_rep(lambda rr: w_rep(rr, rep).start())

    spots = t_r[:, 2, :].astype(I32)
    have = (spots >> 6) == me
    lower = (iota((LANES, LANES), 0) < iota((LANES, LANES), 1)).astype(BF16)
    before = jnp.dot(have.astype(F32).astype(BF16), lower, preferred_element_type=F32).astype(I32)
    ylane = iota((G, LANES), 1)
    code = jnp.where(have, (((spots & 63) + 1) << 7) | ylane, 0)
    codes = [pick(have & (before == k), code) for k in range(CAP)]
    for k in range(CAP):
        rk = jnp.where(codes[k] > 0, codes[k] & 127, -1)
        slotr[k] = jnp.broadcast_to(rk, (G, LANES))
    ecode = jnp.concatenate(codes, axis=0)
    ew = ecode >> 7
    er = ecode & 127
    es = jnp.concatenate([iota((G, 1), 0)] * CAP, axis=0)
    ew_row = to_row(ew)
    used_row = ew_row > 0
    same = (ew == ew_row) & used_row
    rank = jnp.sum(
        jnp.where(same & (iota((nslot, nslot), 1) < iota((nslot, nslot), 0)), 1, 0),
        axis=1,
        keepdims=True,
    )
    rank_row = to_row(rank)
    starts = used_row & ((rank_row & (WIDE - 1)) == 0) & (ew_row < ew)
    base = jnp.sum(jnp.where(starts, 1, 0), axis=1, keepdims=True)
    loc = jnp.where(ew > 0, (base + (rank >> 2)) * WIDE + (rank & (WIDE - 1)), -1)
    loccol[...] = jnp.broadcast_to(loc, (nslot, LANES))
    packed = (ew << 12) | (es << 7) | er
    for b in range(WIDE):
        hit = loc == iota((nslot, LANES), 1) * WIDE + b
        meta_v[b : b + 1, :] = jnp.sum(jnp.where(hit, packed, 0), axis=0, keepdims=True)
    loc_row = to_row(loc)
    for h in range(nslot // LANES):
        meta_v[WIDE + h : WIDE + h + 1, :] = loc_row[:, h * LANES : (h + 1) * LANES]
    plane = iota((nslot, LANES), 1) + 1
    begin = (ew > 0) & ((rank & (WIDE - 1)) == 0)
    first = jnp.sum(jnp.where(begin & (ew < plane), 1, 0), axis=0, keepdims=True)
    held = jnp.sum(jnp.where(begin & (ew == plane), 1, 0), axis=0, keepdims=True)
    meta_v[6:7, :] = jnp.where(held > 0, first + 1, 0)
    meta_v[7:8, :] = jnp.zeros((1, LANES), I32)
    meta_copy = pltpu.make_async_copy(meta_v, meta_s, meta_sem)
    meta_copy.start()
    m_v[...] = jnp.zeros_like(m_v)
    meta_copy.wait()

    finish(q_all, 2 * ZN * (YN - 1), qy_recv)

    def query_of(b, ch):
        return q_all[(meta_s[b, ch] >> 6) & (2 * G - 1)]

    def passage_of(ch):
        return jnp.maximum((meta_s[0, ch] >> 12) - 1, 0)

    token = iota((token_len, LANES), 0)

    def forward(ch):
        pid = passage_of(ch)
        queries = jnp.concatenate([query_of(b, ch) for b in range(WIDE)], axis=0)
        x = lax.dot_general(
            p_v[pid], queries, (((1,), (1,)), ((), ())), preferred_element_type=F32
        )
        x = jnp.where(token < len_ref[0, pid], x, -1e30)
        highest = jnp.max(x, axis=0, keepdims=True)
        powers = jnp.exp2((x - highest) * SCALE2)
        summed = jnp.sum(powers, axis=0, keepdims=True)
        att[ch] = (powers * (1.0 / summed)).astype(BF16)
        return highest + temper * jnp.log(summed)

    def forward_group(g, carry):
        rows = [forward(g * FWD + u) for u in range(FWD)]
        m_v[pl.ds(pl.multiple_of(g * FWD, FWD), FWD), :] = jnp.concatenate(rows, axis=0)
        return carry

    lax.fori_loop(0, NCH // FWD, forward_group, 0)

    matched = m_v[...]
    block = iota((LANES, LANES), 1) >> 5
    loc_cols = loccol[...]
    scores = jnp.zeros((nslot, 1), F32)
    for b in range(WIDE):
        row = to_row(pick(block == b, matched))
        hit = loc_cols == iota((nslot, LANES), 1) * WIDE + b
        scores += pick(hit, jnp.broadcast_to(row, (nslot, LANES)))
    slots = [slotr[k][:, 0:1] for k in range(CAP)]
    score = [scores[k * G : (k + 1) * G, :] for k in range(CAP)]
    belongs = [[(r >= 0) & (r < 64) for r in slots], [r >= 64 for r in slots]]
    spot = ylane - iota((G, LANES), 0)
    stats = jnp.zeros((1, LANES), F32)
    for h in (0, 1):
        top = jnp.full((G, 1), LOW, F32)
        for k in range(CAP):
            top = jnp.maximum(top, jnp.where(belongs[h][k], score[k], LOW))
        total = jnp.zeros((G, 1), F32)
        for k in range(CAP):
            total += jnp.where(belongs[h][k], jnp.exp(score[k] - top), 0.0)
        for col, shift in ((top, h * G), (total, 64 + h * G)):
            stats += jnp.sum(jnp.where(spot == shift, col, 0.0), axis=0, keepdims=True)
    v_r[me] = stats

    def v_to(to, src):
        return remote(v_r.at[src], v_r.at[src], v_sent, v_recv, to, rep)

    def over_all(body):
        over_z(lambda zz: [body(zz * YN + lax.rem(y + t, YN)) for t in (2, 1, 3, 0)] and None, far=True)
        over_y(lambda yy: body(z * YN + yy))

    over_all(lambda g: v_to(g, me).start())

    def lift(ch):
        u = lax.dot_general(
            att[ch], p_v[passage_of(ch)], (((0,), (0,)), ((), ())), preferred_element_type=F32
        )
        u_v[pl.ds(ch * WIDE, WIDE)] = u.astype(BF16).reshape(WIDE, query_len, dim)

    def lift_group(g, carry):
        for u in range(LIFT):
            lift(g * LIFT + u)
        return carry

    groups = NCH // UNROLL
    lax.fori_loop(0, NCH // LIFT, lift_group, 0)

    teacher = t_r[:, 0, :]
    half = ylane >> 6
    top = [jnp.max(jnp.where(half == h, teacher, LOW), axis=1, keepdims=True) for h in (0, 1)]
    shifted = teacher - jnp.where(half == 0, top[0], top[1])
    powers = jnp.exp(shifted)
    total = [pick(half == h, powers) for h in (0, 1)]
    log_teacher = shifted - jnp.log(jnp.where(half == 0, total[0], total[1]))
    weight = [pick(ylane == h * 64, t_r[:, 1, :]) for h in (0, 1)]

    finish(wr, R - 1, w_recv)
    by_rep = jnp.sum(wr[...], axis=0)
    weight_sum = jnp.sum(jnp.where((lane & 63) == 0, by_rep, 0.0), axis=1, keepdims=True)
    finish(v_r, G - 1, v_recv)
    stats = v_r[:, 0, :]
    top = jnp.max(stats, axis=0, keepdims=True)
    total = jnp.sum(pltpu.roll(stats, 64, 1) * jnp.exp(stats - top), axis=0, keepdims=True)
    log_total = top + jnp.log(total)
    log_totals = [pick(spot == h * G, jnp.broadcast_to(log_total, (G, LANES))) for h in (0, 1)]

    scale_all = 2.0 * G * R
    by_slot = []
    part = jnp.zeros((G, 1), F32)
    for k in range(CAP):
        late = belongs[1][k]
        valid = slots[k] >= 0
        log_t = pick(slotr[k] == ylane, log_teacher)
        log_s = score[k] - jnp.where(late, log_totals[1], log_totals[0])
        w = jnp.where(late, weight[1], weight[0])
        prob_t = jnp.exp(log_t)
        grad = scale_all * w / weight_sum * (jnp.exp(log_s) - prob_t)
        grad = jnp.where(valid, grad, 0.0)
        part += jnp.where(valid, w * (prob_t * (log_t - log_s)), 0.0)
        by_slot.append(grad)
        sgq[:, k, :] = jnp.broadcast_to(jnp.where(late, 0.0, grad), (G, LANES))
        sgq[:, CAP + k, :] = jnp.broadcast_to(jnp.where(late, grad, 0.0), (G, LANES))
    g_r[me] = jnp.broadcast_to(jnp.sum(part, axis=0, keepdims=True), (1, LANES))

    def g_to(to):
        return remote(g_r.at[me], g_r.at[me], g_sent, g_recv, to, rep)

    def l_rep(to, src):
        return remote(lr.at[src], lr.at[src], l_sent, l_recv, me, to)

    def query_sum(s):
        scales = sgq[s]
        one = jnp.zeros((query_len, dim), F32)
        two = jnp.zeros((query_len, dim), F32)
        for k in range(CAP):
            e = k * G + s
            at = jnp.maximum(meta_s[WIDE + e // LANES, lax.rem(e, LANES)], 0)
            u = u_v[at].astype(F32)
            one += scales[k : k + 1, :] * u
            two += scales[CAP + k : CAP + k + 1, :] * u
        return one, two

    def o_y(to, zz, src):
        dst = oy_r.at[zz * YN + src]
        return remote(oy_s.at[zz * YN + to], dst, oy_sent, oy_recv.at[zz], z * YN + to, rep)

    def o_z(to, src):
        return remote(oz_s.at[to], oz_r.at[src], oz_sent, oz_recv, to * YN + y, rep)

    def send_sums(zz):
        def one_way(yy):
            one, two = query_sum(zz * YN + yy)
            oy_s[zz * YN + yy, 0] = one.astype(BF16)
            oy_s[zz * YN + yy, 1] = two.astype(BF16)
            o_y(yy, zz, y).start()

        over_y(one_way)

    def send_sums_and_part(zz):
        send_sums(zz)
        for yy in range(YN):
            g_to(zz * YN + yy).start()

    over_z(send_sums_and_part, far=True)
    send_sums(z)
    over_y(lambda yy: g_to(z * YN + yy).start())

    def keep_sums(zz):
        one, two = query_sum(zz * YN + y)
        own[zz, 0] = one
        own[zz, 1] = two

    all_z(keep_sums)

    sg_row = to_row(jnp.concatenate(by_slot, axis=0))
    loc_rows = jnp.concatenate(
        [meta_v[WIDE + h : WIDE + h + 1, :] for h in range(nslot // LANES)], axis=1
    )
    for b in range(WIDE):
        hit = loc_rows == iota((LANES, nslot), 0) * WIDE + b
        col = pick(hit, jnp.broadcast_to(sg_row, (LANES, nslot)))
        sgl[:, b, :] = jnp.broadcast_to(col, (LANES, LANES))

    acc[...] = jnp.zeros_like(acc)

    def back(ch, total):
        scales = sgl[ch]
        scaled = jnp.concatenate(
            [
                (query_of(b, ch).astype(F32) * scales[b : b + 1, :]).astype(BF16)
                for b in range(WIDE)
            ],
            axis=0,
        )
        product = jnp.dot(att[ch], scaled, preferred_element_type=F32)
        follows = (meta_s[0, ch] >> 12) == (meta_s[0, ch + 1] >> 12)
        total = product + total * jnp.where(follows, 1.0, 0.0)
        sums[ch] = total.astype(BF16)
        return total

    def back_group(i, carry):
        g = groups - 1 - i
        total = acc[...]
        for u in range(UNROLL):
            total = back(g * UNROLL + UNROLL - 1 - u, total)
        acc[...] = total
        return carry

    def line_sum(zz):
        finish(oy_r, YN - 1, oy_recv.at[zz])
        total = own[zz]
        for t in range(1, YN):
            total += oy_r[zz * YN + lax.rem(y + t, YN)].astype(F32)
        return total

    def send_line(zz):
        oz_s[zz] = line_sum(zz).astype(BF16)
        o_z(zz, z).start()

    share = groups // (ZN - 1)

    def send_between(t, carry):
        lax.fori_loop((t - 1) * share, t * share, back_group, 0)
        send_line(near_z(ZN - t))
        return carry

    lax.fori_loop(1, ZN, send_between, 0)
    lax.fori_loop(share * (ZN - 1), groups, back_group, 0)
    own[z] = line_sum(z)
    finish(g_r, G - 1, g_recv)
    lr[rep] = jnp.sum(g_r[...], axis=0)
    over_rep(lambda rr: l_rep(rr, rep).start())

    def place(i, carry):
        for u in range(8):
            p = i * 8 + u
            mark = meta_s[6, p]
            rows = sums[jnp.maximum(mark - 1, 0)].astype(F32) * jnp.where(mark > 0, 1.0, 0.0)
            p_f[pl.ds(p, token_len, stride=stored), :] = rows
        return carry

    lax.fori_loop(0, stored // 8, place, 0)

    def pack(i, carry):
        for u in range(12):
            j = i * 12 + u
            pgrad_ref[j] = p_f[pl.ds(pl.multiple_of(j * stored, stored), stored), :].astype(BF16)
        return carry

    lax.fori_loop(0, token_len // 12, pack, 0)

    finish(t_r, G - 1, t_sent)
    finish(q_all, 2 * (G - 1), q_sent)
    finish(v_r, G - 1, v_sent)
    finish(g_r, G - 1, g_sent)
    finish(oy_s, ZN * (YN - 1), oy_sent)
    finish(oz_s, ZN - 1, oz_sent)
    finish(wr, R - 1, w_sent)
    finish(lr, R - 1, l_sent)

    finish(lr, R - 1, l_recv)
    loss_ref[...] = jnp.sum(lr[...], axis=0) / weight_sum

    finish(oz_r, ZN - 1, oz_recv)
    total = own[z]
    for t in range(1, ZN):
        total += oz_r[lax.rem(z + t, ZN)].astype(F32)
    qgrad_ref[...] = total


def on_device(G, R, queries, passages, lengths, cand_ids, owner_map, teacher, weights):
    query_local, _, query_len, dim = queries.shape
    stored, _, token_len, _ = passages.shape
    chunks = (G * CAP + (WIDE - 1) * stored) // WIDE
    NCH = -(-chunks // UNROLL) * UNROLL
    pitch = -(-token_len // 8) * 8
    ZN = G // YN
    vmem = pl.BlockSpec(memory_space=pltpu.VMEM)
    hbm = pl.BlockSpec(memory_space=pl.ANY)
    dma = pltpu.SemaphoreType.DMA
    loss, qgrad, pgrad = pl.pallas_call(
        functools.partial(step_kernel, G, R, NCH),
        out_shape=(
            pltpu.VMEM((1, LANES), F32),
            pltpu.VMEM((query_local, query_len, dim), F32),
            pltpu.VMEM((token_len, stored, dim), BF16),
        ),
        in_specs=[hbm] * 7,
        out_specs=(vmem, vmem, vmem),
        scratch_shapes=[
            pltpu.VMEM(cand_ids.shape, I32),
            pltpu.VMEM(owner_map.shape, I32),
            pltpu.VMEM((query_local, query_len, dim), BF16),
            pltpu.SMEM((1, stored), I32),
            pltpu.VMEM(teacher.shape, F32),
            pltpu.SMEM((1, query_local), F32),
            pltpu.VMEM((token_len, stored, dim), BF16),
            pltpu.VMEM((stored * pitch, dim), F32),
            pltpu.VMEM((stored, token_len, dim), BF16),
            pltpu.VMEM((query_local * G, query_len, dim), BF16),
            pltpu.VMEM((1, LANES), I32),
            pltpu.VMEM((G, 3, LANES), F32),
            pltpu.VMEM((G, 1, LANES), F32),
            pltpu.VMEM((G, 1, LANES), F32),
            pltpu.VMEM((R, 1, LANES), F32),
            pltpu.VMEM((R, 1, LANES), F32),
            pltpu.VMEM((8, LANES), I32),
            pltpu.SMEM((8, LANES), I32),
            pltpu.VMEM((LANES, LANES), F32),
            pltpu.VMEM((NCH, token_len, LANES), BF16),
            pltpu.VMEM((NCH * WIDE, query_len, dim), BF16),
            pltpu.VMEM((CAP, G, LANES), I32),
            pltpu.VMEM((G * CAP, LANES), I32),
            pltpu.VMEM((G, 2 * CAP, LANES), F32),
            pltpu.VMEM((LANES, WIDE, LANES), F32),
            pltpu.VMEM((G, query_local, query_len, dim), BF16),
            pltpu.VMEM((G, query_local, query_len, dim), BF16),
            pltpu.VMEM((ZN, query_local, query_len, dim), BF16),
            pltpu.VMEM((ZN, query_local, query_len, dim), BF16),
            pltpu.VMEM((ZN, query_local, query_len, dim), F32),
            pltpu.VMEM((NCH, token_len, dim), BF16),
            pltpu.VMEM((token_len, dim), F32),
            dma((6,)),
            dma,
            dma,
        ]
        + [dma] * 15
        + [dma((ZN,))] * 3,
        compiler_params=pltpu.CompilerParams(
            collective_id=0, has_side_effects=True, vmem_limit_bytes=56 * 1024 * 1024
        ),
    )(
        cand_ids,
        owner_map,
        queries.reshape(query_local, query_len, dim),
        jnp.transpose(passages[:, 0], (1, 0, 2)),
        lengths.reshape(1, stored),
        teacher,
        weights.reshape(1, query_local),
    )
    return loss[0, 0], qgrad[:, None], jnp.transpose(pgrad, (1, 0, 2))[:, None]


def solution(mesh):
    G, R = mesh.shape["grp"], mesh.shape["rep"]
    in_specs = (
        P("grp", "rep", None, None),
        P("grp", "rep", None, None),
        P("grp", "rep"),
        P("grp", "rep", None),
        P("rep", None),
        P("grp", "rep", None),
        P("grp", "rep"),
    )
    out_specs = (P(), P("grp", "rep", None, None), P("grp", "rep", None, None))
    return jax.shard_map(
        functools.partial(on_device, G, R),
        mesh=mesh,
        in_specs=in_specs,
        out_specs=out_specs,
        check_vma=False,
    )
```
